16 devices in a mesh: replica: 4 (over z, y), model: 4 (over x, core).
Axes of the slice: x: 2, y: 2, z: 2, core: 2. Of those that a mesh axis runs over, the one named last changes fastest.
Arguments:
- x: bfloat16 [512, 2048], P('replica'), parts along dimension 0
- cache_len: int32 [512], P('replica'), parts along dimension 0
- w_query: bfloat16 [2, 2048, 2048], P(None, None, 'model')
- w_key: bfloat16 [2, 2048, 256], replicated
- w_value: bfloat16 [2, 2048, 256], replicated
- w_out: bfloat16 [2, 2048, 2048], P(None, 'model')
- k_cache: bfloat16 [2, 512, 512, 256], P(None, ('replica', 'model')), parts along dimension 1
- v_cache: bfloat16 [2, 512, 512, 256], P(None, ('replica', 'model')), parts along dimension 1
Outputs:
- output 1: bfloat16 [512, 2048], P('replica'), parts along dimension 0
- output 2: bfloat16 [2, 512, 512, 256], P(None, ('replica', 'model')), parts along dimension 1
- output 3: bfloat16 [2, 512, 512, 256], P(None, ('replica', 'model')), parts along dimension 1
There are 4 independent parts. The reference program is written for one: setup_inputs(seed, part) draws one part's arguments, and reference() takes and returns one part's arrays. A program takes and returns all parts, laid end to end along the dimension named above; an argument that names none is the same for every part.
All inputs are finite; a program needn't handle non-finite values.
Results may differ from the reference program's by a relative error of at most 0.00437.
Values are sent between devices in bfloat16 or wider.
A program may use at most 1 GiB of HBM per device.

```python
import jax
import jax.numpy as jnp
from jax import lax

LAYERS = 2
BATCH = 128
D_MODEL = 2048
NUM_HEADS = 8
HEAD_DIM = 256
SEQ_LEN = 512

SEQ_BITS = SEQ_LEN.bit_length() - 1
Q_WIDTH = NUM_HEADS * HEAD_DIM


def setup_inputs(seed: int = 0, part: int = 0) -> dict:
    root_key = jax.random.key(seed)
    shared = jax.random.split(root_key, 4)
    part_keys = jax.random.split(jax.random.fold_in(root_key, part), 6)
    x = jax.random.normal(part_keys[0], (BATCH, D_MODEL), jnp.float32).astype(jnp.bfloat16)
    raw_len = jax.random.randint(part_keys[1], (BATCH,), 0, SEQ_LEN)
    shift_by = jax.random.randint(part_keys[2], (BATCH,), 0, SEQ_BITS + 1)
    row_order = jax.random.permutation(part_keys[3], BATCH)
    cache_len = jnp.right_shift(raw_len, shift_by)
    cache_len = cache_len.at[row_order[0]].set(SEQ_LEN - 1).at[row_order[1]].set(0)
    w_query = (1.5 * D_MODEL ** -0.5) * jax.random.normal(shared[0], (LAYERS, D_MODEL, Q_WIDTH), jnp.float32)
    w_key = (1.5 * D_MODEL ** -0.5) * jax.random.normal(shared[1], (LAYERS, D_MODEL, HEAD_DIM), jnp.float32)
    w_value = (D_MODEL ** -0.5) * jax.random.normal(shared[2], (LAYERS, D_MODEL, HEAD_DIM), jnp.float32)
    w_out = (2.0 * Q_WIDTH ** -0.5) * jax.random.normal(shared[3], (LAYERS, Q_WIDTH, D_MODEL), jnp.float32)
    k_cache = 1.5 * jax.random.normal(part_keys[4], (LAYERS, BATCH, SEQ_LEN, HEAD_DIM), jnp.float32)
    v_cache = jax.random.normal(part_keys[5], (LAYERS, BATCH, SEQ_LEN, HEAD_DIM), jnp.float32)
    return {
        "x": x,
        "cache_len": cache_len,
        "w_query": w_query.astype(jnp.bfloat16),
        "w_key": w_key.astype(jnp.bfloat16),
        "w_value": w_value.astype(jnp.bfloat16),
        "w_out": w_out.astype(jnp.bfloat16),
        "k_cache": k_cache.astype(jnp.bfloat16),
        "v_cache": v_cache.astype(jnp.bfloat16),
    }


def attend_layer(hidden, cache_len, query_w, key_w, value_w, out_w, k_layer, v_layer):
    query = jnp.dot(hidden, query_w, preferred_element_type=jnp.float32).astype(jnp.bfloat16)
    query = query.reshape(BATCH, NUM_HEADS, HEAD_DIM)
    k_new = jnp.dot(hidden, key_w, preferred_element_type=jnp.float32).astype(jnp.bfloat16)
    v_new = jnp.dot(hidden, value_w, preferred_element_type=jnp.float32).astype(jnp.bfloat16)
    write_here = jnp.arange(SEQ_LEN)[None, :, None] == cache_len[:, None, None]
    k_layer = jnp.where(write_here, k_new[:, None, :], k_layer)
    v_layer = jnp.where(write_here, v_new[:, None, :], v_layer)

    def one_row(row_items):
        q_row, k_row, v_row, row_len = row_items
        scores = jnp.dot(q_row, k_row.T, preferred_element_type=jnp.float32) * (HEAD_DIM ** -0.5)
        visible = jnp.arange(SEQ_LEN)[None, :] <= row_len
        scores = jnp.where(visible, scores, -jnp.inf)
        weights = jax.nn.softmax(scores, axis=-1).astype(jnp.bfloat16)
        context = jnp.dot(weights, v_row, preferred_element_type=jnp.float32)
        return context.astype(jnp.bfloat16)

    context = lax.map(one_row, (query, k_layer, v_layer, cache_len))
    update = jnp.dot(context.reshape(BATCH, Q_WIDTH), out_w, preferred_element_type=jnp.float32)
    hidden = (hidden.astype(jnp.float32) + update).astype(jnp.bfloat16)
    return hidden, k_layer, v_layer


def reference(x, cache_len, w_query, w_key, w_value, w_out, k_cache, v_cache):
    def layer_step(hidden, params):
        query_w, key_w, value_w, out_w, k_layer, v_layer = params
        hidden, k_layer, v_layer = attend_layer(hidden, cache_len, query_w, key_w, value_w, out_w, k_layer, v_layer)
        return hidden, (k_layer, v_layer)

    out, (k_all, v_all) = lax.scan(layer_step, x, (w_query, w_key, w_value, w_out, k_cache, v_cache))
    return out, k_all, v_all
```

```python
import functools

import jax
import jax.numpy as jnp
from jax import lax
from jax.experimental import pallas as pl
from jax.experimental.pallas import tpu as pltpu
from jax.sharding import PartitionSpec as P

F32 = jnp.float32
BF16 = jnp.bfloat16
MESH = pl.DeviceIdType.MESH
HBM = pl.BlockSpec(memory_space=pltpu.HBM)
VM = pl.BlockSpec(memory_space=pltpu.VMEM)
SM = pl.BlockSpec(memory_space=pltpu.SMEM)
DMA = pltpu.SemaphoreType.DMA


def dot(a, b):
    return jnp.dot(a, b, preferred_element_type=F32)


def place():
    m = lax.axis_index("model")
    return lax.axis_index("replica"), m, lax.rem(m, 2), m // 2


def meet(peers):
    barrier = pltpu.get_barrier_semaphore()
    for peer in peers:
        pl.semaphore_signal(barrier, inc=1, device_id=peer, device_id_type=MESH)
    pl.semaphore_wait(barrier, len(peers))


def send(src, dst, send_sem, recv_sem, peer):
    return pltpu.make_async_remote_copy(
        src_ref=src, dst_ref=dst, send_sem=send_sem, recv_sem=recv_sem, device_id=peer, device_id_type=MESH)


def first_kernel(x_hbm, wq_hbm, wk_hbm, wv_hbm, kc_hbm, vc_hbm,
                 q_out, kn_out, vn_out, kb, vb,
                 xs, wqs, wks, wvs, qown, qrecv,
                 wsem, csem, qsend, qrecv_sem):
    rep, m, core, chip = place()
    rows = q_out.shape[1]
    across, diag, mate = (rep, lax.rem(m + 2, 4)), (rep, 3 - m), (rep, m + 1 - 2 * core)
    loads = [pltpu.make_async_copy(x_hbm, xs, wsem.at[0])]
    for i in range(2):
        loads.append(pltpu.make_async_copy(wq_hbm.at[0, :, pl.ds(i * 256, 256)], wqs.at[i], wsem.at[1 + i]))
    loads.append(pltpu.make_async_copy(wk_hbm.at[0], wks, wsem.at[3]))
    loads.append(pltpu.make_async_copy(wv_hbm.at[0], wvs, wsem.at[4]))
    for load in loads:
        load.start()
    caches = [pltpu.make_async_copy(kc_hbm.at[0], kb, csem.at[0]), pltpu.make_async_copy(vc_hbm.at[0], vb, csem.at[1])]
    meet((across, diag, mate))
    loads[0].wait()
    copies = []
    for i in range(2):
        loads[1 + i].wait()
        if i == 1:
            for c in caches:
                c.start()
        q = dot(xs[...], wqs[i]).astype(BF16)
        for d in range(4):
            qown[d, i] = q[d * rows:(d + 1) * rows]
        for n, (peer, who) in enumerate(((across, lax.rem(m + 2, 4)), (diag, 3 - m), (mate, m + 1 - 2 * core))):
            c = send(qown.at[who, i], qrecv.at[m, i], qsend.at[n, i], qrecv_sem.at[n, i], peer)
            c.start()
            copies.append(c)
        qrecv[m, i] = qown[m, i]
    mine = xs[pl.ds(pl.multiple_of(m * rows, rows), rows), :]
    loads[3].wait()
    kn_out[...] = dot(mine, wks[...]).astype(BF16).astype(F32)
    loads[4].wait()
    vn_out[...] = dot(mine, wvs[...]).astype(BF16).astype(F32)
    for c in copies:
        c.wait()
    for s in range(4):
        for i in range(2):
            q_out[2 * s + i] = qrecv[s, i]
    for c in caches:
        c.wait()


def attend_kernel(*refs, layer):
    if layer:
        len_ref, q_ref, kn, vn, kb, vb, _, _, ctx, _, _, ko, vo, qs, st, acc, osem = refs
    else:
        len_ref, q_ref, kn, vn, kb, vb, ctx, _, _, ko, vo, qs, st, acc, osem = refs
    heads, rows, dim = q_ref.shape
    seq = kb.shape[1]
    base = lax.axis_index("model") * rows
    half = 16

    def patch(b, carry):
        ln = len_ref[base + b]
        start = pl.multiple_of((ln // half) * half, half)
        hit = lax.broadcasted_iota(jnp.int32, (half, dim), 0) == ln - start
        for buf, new in ((kb, kn), (vb, vn)):
            old = buf[b, pl.ds(start, half), :].astype(F32)
            buf[b, pl.ds(start, half), :] = jnp.where(hit, new[pl.ds(b, 1), :], old).astype(BF16)
        return carry

    lax.fori_loop(0, rows, patch, 0, unroll=4)
    outs = []
    step = 4
    for i in range(rows // step):
        for n, (src, dst) in enumerate(((kb, ko), (vb, vo))):
            c = pltpu.make_async_copy(src.at[pl.ds(i * step, step)], dst.at[layer, pl.ds(i * step, step)], osem.at[n, i])
            c.start()
            outs.append(c)
    lanes = heads * half
    lane_b = lax.rem(lax.broadcasted_iota(jnp.int32, (1, lanes), 1), half)
    row_b = lax.rem(lax.broadcasted_iota(jnp.int32, (lanes, 1), 0), half)
    pos = lax.broadcasted_iota(jnp.int32, (seq, lanes), 0)
    for g in range(rows // half):
        for h in range(heads):
            qs[h * half:(h + 1) * half, :] = q_ref[h, g * half:(g + 1) * half, :]
        lens = jnp.zeros((1, lanes), jnp.int32)
        for b in range(half):
            lens = jnp.where(lane_b == b, len_ref[base + g * half + b], lens)

        def scores(b, carry):
            s = lax.dot_general(kb[g * half + b], qs[...], (((1,), (1,)), ((), ())), preferred_element_type=F32)
            st[...] = jnp.where(lane_b == b, s, st[...])
            return carry

        lax.fori_loop(0, half, scores, 0, unroll=2)
        s = jnp.where(pos <= lens, st[...] * (dim ** -0.5), -jnp.inf)
        e = jnp.exp(s - jnp.max(s, axis=0, keepdims=True))
        p = e * (1.0 / jnp.sum(e, axis=0, keepdims=True))
        p = p.T.astype(BF16)

        def mix(b, carry):
            c = dot(p, vb[g * half + b])
            acc[...] = jnp.where(row_b == b, c, acc[...])
            return carry

        lax.fori_loop(0, half, mix, 0, unroll=2)
        for h in range(heads):
            ctx[h, g * half:(g + 1) * half, :] = acc[h * half:(h + 1) * half, :].astype(BF16)
    for c in outs:
        c.wait()


def exchange_kernel(*refs, layer, last):
    if last:
        (ctx, hid, wo_hbm, out,
         wos, lhs, ys, yrecv, hl, pown, pfwd,
         wsem, csem, ysem, hsem, psem, fsem) = refs
    else:
        (ctx, x_hbm, wo_hbm, wq_hbm, wk_hbm, wv_hbm, kc_hbm, vc_hbm,
         q_out, kn_out, vn_out, hid_out, kb, vb,
         wos, lhs, ys, yrecv, hl, xs, wqs, wks, wvs, qacc, qown, qrecv,
         wsem, csem, ysem, hsem, qsem, kvsem) = refs
    rep, m, core, chip = place()
    across_m, mate_m = lax.rem(m + 2, 4), m + 1 - 2 * core
    across, mate = (rep, across_m), (rep, mate_m)
    rows = ctx.shape[1]
    chunks = hl.shape[0]
    load_wo = pltpu.make_async_copy(wo_hbm.at[layer], wos.at[core], wsem.at[0])
    load_wo.start()
    if not last:
        load_x = pltpu.make_async_copy(x_hbm.at[pl.ds(pl.multiple_of(m * rows, rows), rows)], xs, wsem.at[1])
        load_q = pltpu.make_async_copy(wq_hbm.at[layer + 1], wqs.at[core], wsem.at[2])
        load_k = pltpu.make_async_copy(wk_hbm.at[layer + 1], wks, wsem.at[3])
        load_v = pltpu.make_async_copy(wv_hbm.at[layer + 1], wvs, wsem.at[4])
        for c in (load_x, load_q, load_k, load_v):
            c.start()
    meet((across, mate))
    give = send(ctx.at[pl.ds((1 - chip) * 4, 4)], lhs.at[:, pl.ds(rows, rows), :], csem.at[0], csem.at[1], across)
    give.start()
    load_wo.wait()
    push_wo = send(wos.at[core], wos.at[core], wsem.at[5], wsem.at[6], mate)
    push_wo.start()
    if not last:
        load_q.wait()
        push_q = send(wqs.at[core], wqs.at[core], wsem.at[7], wsem.at[8], mate)
        push_q.start()
        caches = [pltpu.make_async_copy(kc_hbm.at[layer + 1], kb, kvsem.at[0]),
                  pltpu.make_async_copy(vc_hbm.at[layer + 1], vb, kvsem.at[1])]
        for c in caches:
            c.start()
    for i in range(4):
        lhs[i, 0:rows, :] = ctx[chip * 4 + i]
    give.wait()
    push_wo.wait()
    ycopies = []
    for j in range(chunks):
        y = dot(lhs[0], wos[0, 0:256, j * 256:(j + 1) * 256])
        for i in range(1, 4):
            y += dot(lhs[i], wos[i // 2, (i % 2) * 256:(i % 2 + 1) * 256, j * 256:(j + 1) * 256])
        ys[j] = y
        c = send(ys.at[j, pl.ds(rows, rows)], yrecv.at[j], ysem.at[0, j], ysem.at[1, j], across)
        c.start()
        ycopies.append(c)
    if not last:
        load_x.wait()
    hcopies = []
    pcopies = []
    for j in range(chunks):
        ycopies[j].wait_recv()
        old = hid[j] if last else xs[:, j * 256:(j + 1) * 256]
        new = (old.astype(F32) + (ys[j, 0:rows, :] + yrecv[j])).astype(BF16)
        hl[j, 0:rows, :] = new
        c = send(hl.at[j, pl.ds(0, rows)], hl.at[j, pl.ds(rows, rows)], hsem.at[0, j], hsem.at[1, j], across)
        c.start()
        hcopies.append(c)
        if last:
            c = send(hl.at[j, pl.ds(0, rows)], pown.at[j], psem.at[0, j], psem.at[1, j], mate)
            c.start()
            pcopies.append(c)
    if last:
        fcopies = []
        for j in range(chunks):
            hcopies[j].wait_recv()
            c = send(hl.at[j, pl.ds(rows, rows)], pfwd.at[j], fsem.at[0, j], fsem.at[1, j], mate)
            c.start()
            fcopies.append(c)
        for j in range(chunks):
            cols = slice(j * 256, (j + 1) * 256)
            out[pl.ds(pl.multiple_of(m * rows, rows), rows), cols] = hl[j, 0:rows, :]
            out[pl.ds(pl.multiple_of(across_m * rows, rows), rows), cols] = hl[j, rows:2 * rows, :]
        for j in range(chunks):
            cols = slice(j * 256, (j + 1) * 256)
            pcopies[j].wait_recv()
            out[pl.ds(pl.multiple_of(mate_m * rows, rows), rows), cols] = pown[j]
            fcopies[j].wait_recv()
            out[pl.ds(pl.multiple_of((3 - m) * rows, rows), rows), cols] = pfwd[j]
        for c in ycopies + hcopies + pcopies + fcopies:
            c.wait_send()
        return
    push_q.wait()
    for j in range(chunks):
        hcopies[j].wait_recv()
        for i in range(4):
            part = dot(hl[j], wqs[i // 2, j * 256:(j + 1) * 256, (i % 2) * 256:(i % 2 + 1) * 256])
            if j == 0:
                qacc[i] = part
            else:
                qacc[i] += part
    qcopies = []
    for i in range(4):
        qown[i] = qacc[i].astype(BF16)
        c = send(qown.at[i, pl.ds(rows, rows)], qrecv.at[i], qsem.at[0, i], qsem.at[1, i], across)
        c.start()
        qcopies.append(c)
    for load, w, res in ((load_k, wks, kn_out), (load_v, wvs, vn_out)):
        load.wait()
        t = dot(hl[0, 0:rows, :], w[0:256, :])
        for j in range(1, chunks):
            t += dot(hl[j, 0:rows, :], w[j * 256:(j + 1) * 256, :])
        res[...] = t.astype(BF16).astype(F32)
    for j in range(chunks):
        hid_out[j] = hl[j, 0:rows, :]
    for i in range(4):
        q_out[chip * 4 + i] = qown[i, 0:rows, :]
    for i in range(4):
        qcopies[i].wait_recv()
        q_out[(1 - chip) * 4 + i] = qrecv[i]
    for c in ycopies + hcopies + qcopies:
        c.wait_send()
    for c in caches:
        c.wait()


def solution(mesh):
    groups = mesh.shape["model"]
    row_axes = ("replica", "model")
    cache_spec = P(None, row_axes, None, None)

    def device_step(x, cache_len, w_query, w_key, w_value, w_out, k_cache, v_cache):
        layers, rows, seq, dim = k_cache.shape
        total, width = x.shape
        chunks = width // dim
        heads = w_query.shape[-1] // dim * groups
        local = w_query.shape[-1]
        hd = (heads, rows, dim)
        x, w_query, w_key, w_value, w_out, k_cache, v_cache = (
            pltpu.with_memory_space_constraint(a, pltpu.HBM)
            for a in (x, w_query, w_key, w_value, w_out, k_cache, v_cache))
        remote = functools.partial(pltpu.CompilerParams, has_side_effects=True)

        q, kn, vn, kb, vb = pl.pallas_call(
            first_kernel,
            out_shape=(pltpu.VMEM(hd, BF16), pltpu.VMEM((rows, dim), F32), pltpu.VMEM((rows, dim), F32),
                       pltpu.VMEM((rows, seq, dim), BF16), pltpu.VMEM((rows, seq, dim), BF16)),
            in_specs=[HBM] * 6,
            out_specs=(VM,) * 5,
            scratch_shapes=[
                pltpu.VMEM((total, width), BF16), pltpu.VMEM((2, width, dim), BF16),
                pltpu.VMEM((width, dim), BF16), pltpu.VMEM((width, dim), BF16),
                pltpu.VMEM((4, 2, rows, dim), BF16), pltpu.VMEM((4, 2, rows, dim), BF16),
                DMA((5,)), DMA((2,)), DMA((3, 2)), DMA((3, 2)),
            ],
            compiler_params=remote(collective_id=0, vmem_limit_bytes=16 << 20),
            name="first",
        )(x, w_query, w_key, w_value, k_cache, v_cache)

        ko = vo = None
        hid = x
        for layer in range(layers):
            last = layer == layers - 1
            ins = (cache_len, q, kn, vn, kb, vb) + ((ko, vo) if layer else ())
            ctx, _, _, ko, vo = pl.pallas_call(
                functools.partial(attend_kernel, layer=layer),
                out_shape=(pltpu.VMEM(hd, BF16), pltpu.VMEM(kb.shape, BF16), pltpu.VMEM(vb.shape, BF16),
                           jax.ShapeDtypeStruct(k_cache.shape, BF16), jax.ShapeDtypeStruct(v_cache.shape, BF16)),
                in_specs=[SM] + [VM] * 5 + ([HBM, HBM] if layer else []),
                out_specs=(VM, VM, VM, HBM, HBM),
                input_output_aliases={4: 1, 5: 2, 6: 3, 7: 4} if layer else {4: 1, 5: 2},
                scratch_shapes=[
                    pltpu.VMEM((heads * 16, dim), BF16), pltpu.VMEM((seq, heads * 16), F32),
                    pltpu.VMEM((heads * 16, dim), F32), DMA((2, rows // 4)),
                ],
                compiler_params=pltpu.CompilerParams(vmem_limit_bytes=8 << 20),
                name=f"attend{layer}",
            )(*ins)
            common = [
                pltpu.VMEM((2, local, width), BF16), pltpu.VMEM((4, 2 * rows, dim), BF16),
                pltpu.VMEM((chunks, 2 * rows, dim), F32), pltpu.VMEM((chunks, rows, dim), F32),
                pltpu.VMEM((chunks, 2 * rows, dim), BF16),
            ]
            sems = [DMA((9,)), DMA((2,)), DMA((2, chunks)), DMA((2, chunks))]
            if last:
                out = pl.pallas_call(
                    functools.partial(exchange_kernel, layer=layer, last=True),
                    out_shape=pltpu.VMEM((total, width), BF16),
                    in_specs=[VM, VM, HBM],
                    out_specs=VM,
                    scratch_shapes=common + [pltpu.VMEM((chunks, rows, dim), BF16)] * 2
                    + sems + [DMA((2, chunks)), DMA((2, chunks))],
                    compiler_params=remote(collective_id=layer + 1, vmem_limit_bytes=16 << 20),
                    name="last",
                )(ctx, hid, w_out)
            else:
                q, kn, vn, hid, kb, vb = pl.pallas_call(
                    functools.partial(exchange_kernel, layer=layer, last=False),
                    out_shape=(pltpu.VMEM(hd, BF16), pltpu.VMEM((rows, dim), F32), pltpu.VMEM((rows, dim), F32),
                               pltpu.VMEM((chunks, rows, dim), BF16),
                               pltpu.VMEM((rows, seq, dim), BF16), pltpu.VMEM((rows, seq, dim), BF16)),
                    in_specs=[VM] + [HBM] * 7,
                    out_specs=(VM,) * 6,
                    scratch_shapes=common + [
                        pltpu.VMEM((rows, width), BF16), pltpu.VMEM((2, width, local), BF16),
                        pltpu.VMEM((width, dim), BF16), pltpu.VMEM((width, dim), BF16),
                        pltpu.VMEM((4, 2 * rows, dim), F32), pltpu.VMEM((4, 2 * rows, dim), BF16),
                        pltpu.VMEM((4, rows, dim), BF16),
                    ] + sems + [DMA((2, 4)), DMA((2,))],
                    compiler_params=remote(collective_id=layer + 1, vmem_limit_bytes=24 << 20),
                    name="middle",
                )(ctx, hid, w_out, w_query, w_key, w_value, k_cache, v_cache)
        return out, ko, vo

    return jax.shard_map(
        device_step,
        mesh=mesh,
        in_specs=(P("replica", None), P("replica"), P(None, None, "model"), P(), P(), P(None, "model", None), cache_spec, cache_spec),
        out_specs=(P("replica", None), cache_spec, cache_spec),
        check_vma=False,
    )
```

```python
import functools

import jax
import jax.numpy as jnp
from jax import lax
from jax.experimental import pallas as pl
from jax.experimental.pallas import tpu as pltpu
from jax.sharding import PartitionSpec as P

F32 = jnp.float32
BF16 = jnp.bfloat16
MESH = pl.DeviceIdType.MESH
HBM = pl.BlockSpec(memory_space=pltpu.HBM)
VM = pl.BlockSpec(memory_space=pltpu.VMEM)
SM = pl.BlockSpec(memory_space=pltpu.SMEM)
DMA = pltpu.SemaphoreType.DMA


def dot(a, b):
    return jnp.dot(a, b, preferred_element_type=F32)


def place():
    m = lax.axis_index("model")
    return lax.axis_index("replica"), m, lax.rem(m, 2), m // 2


def meet(peers):
    barrier = pltpu.get_barrier_semaphore()
    for peer in peers:
        pl.semaphore_signal(barrier, inc=1, device_id=peer, device_id_type=MESH)
    pl.semaphore_wait(barrier, len(peers))


def send(src, dst, send_sem, recv_sem, peer):
    return pltpu.make_async_remote_copy(
        src_ref=src, dst_ref=dst, send_sem=send_sem, recv_sem=recv_sem, device_id=peer, device_id_type=MESH)


def first_kernel(x_hbm, wq_hbm, wk_hbm, wv_hbm, kc_hbm, vc_hbm,
                 q_out, kn_out, vn_out, kb, vb,
                 xs, wqs, wks, wvs, qown, qrecv,
                 wsem, csem, qsend, qrecv_sem):
    rep, m, core, chip = place()
    rows = q_out.shape[1]
    across, diag, mate = (rep, lax.rem(m + 2, 4)), (rep, 3 - m), (rep, m + 1 - 2 * core)
    loads = [pltpu.make_async_copy(x_hbm, xs, wsem.at[0])]
    for i in range(2):
        loads.append(pltpu.make_async_copy(wq_hbm.at[0, :, pl.ds(i * 256, 256)], wqs.at[i], wsem.at[1 + i]))
    loads.append(pltpu.make_async_copy(wk_hbm.at[0], wks, wsem.at[3]))
    loads.append(pltpu.make_async_copy(wv_hbm.at[0], wvs, wsem.at[4]))
    for load in loads:
        load.start()
    caches = [pltpu.make_async_copy(kc_hbm.at[0], kb, csem.at[0]), pltpu.make_async_copy(vc_hbm.at[0], vb, csem.at[1])]
    meet((across, diag, mate))
    loads[0].wait()
    copies = []
    for i in range(2):
        loads[1 + i].wait()
        if i == 1:
            for c in caches:
                c.start()
        q = dot(xs[...], wqs[i]).astype(BF16)
        for d in range(4):
            qown[d, i] = q[d * rows:(d + 1) * rows]
        for n, (peer, who) in enumerate(((across, lax.rem(m + 2, 4)), (diag, 3 - m), (mate, m + 1 - 2 * core))):
            c = send(qown.at[who, i], qrecv.at[m, i], qsend.at[n, i], qrecv_sem.at[n, i], peer)
            c.start()
            copies.append(c)
        qrecv[m, i] = qown[m, i]
    mine = xs[pl.ds(pl.multiple_of(m * rows, rows), rows), :]
    loads[3].wait()
    kn_out[...] = dot(mine, wks[...]).astype(BF16).astype(F32)
    loads[4].wait()
    vn_out[...] = dot(mine, wvs[...]).astype(BF16).astype(F32)
    for c in copies:
        c.wait()
    for s in range(4):
        for i in range(2):
            q_out[2 * s + i] = qrecv[s, i]
    for c in caches:
        c.wait()


def attend_kernel(*refs, layer):
    if layer:
        len_ref, q_ref, kn, vn, kb, vb, _, _, ctx, _, _, ko, vo, qs, st, osem = refs
    else:
        len_ref, q_ref, kn, vn, kb, vb, ctx, _, _, ko, vo, qs, st, osem = refs
    heads, rows, dim = q_ref.shape
    seq = kb.shape[1]
    base = lax.axis_index("model") * rows
    half = 16

    def patch(b, carry):
        ln = len_ref[base + b]
        start = pl.multiple_of((ln // half) * half, half)
        hit = lax.broadcasted_iota(jnp.int32, (half, dim), 0) == ln - start
        for buf, new in ((kb, kn), (vb, vn)):
            old = buf[b, pl.ds(start, half), :].astype(F32)
            buf[b, pl.ds(start, half), :] = jnp.where(hit, new[pl.ds(b, 1), :], old).astype(BF16)
        return carry

    lax.fori_loop(0, rows, patch, 0, unroll=4)
    outs = []
    step = 16
    for i in range(rows // step):
        for n, (src, dst) in enumerate(((kb, ko), (vb, vo))):
            c = pltpu.make_async_copy(src.at[pl.ds(i * step, step)], dst.at[layer, pl.ds(i * step, step)], osem.at[n, i])
            c.start()
            outs.append(c)
    for h in range(heads):
        for i in range(dim // 128):
            qs[i, pl.ds(h, rows, stride=heads), :] = q_ref[h, :, i * 128:(i + 1) * 128].astype(F32)
    pos = lax.broadcasted_iota(jnp.int32, (heads, seq), 1)
    for b in range(rows):
        q = jnp.concatenate([qs[i, b * heads:(b + 1) * heads, :] for i in range(dim // 128)], axis=1).astype(BF16)
        s = lax.dot_general(q, kb[b], (((1,), (1,)), ((), ())), preferred_element_type=F32)
        st[b * heads:(b + 1) * heads, :] = jnp.where(pos <= len_ref[base + b], s * (dim ** -0.5), -jnp.inf)
    for b in range(rows):
        s = st[b * heads:(b + 1) * heads, :]
        e = jnp.exp(s - jnp.max(s, axis=1, keepdims=True))
        p = (e * (1.0 / jnp.sum(e, axis=1, keepdims=True))).astype(BF16)
        c = dot(p, vb[b])
        for i in range(dim // 128):
            qs[i, b * heads:(b + 1) * heads, :] = c[:, i * 128:(i + 1) * 128]
    for h in range(heads):
        for i in range(dim // 128):
            ctx[h, :, i * 128:(i + 1) * 128] = qs[i, pl.ds(h, rows, stride=heads), :].astype(BF16)
    for c in outs:
        c.wait()


def exchange_kernel(*refs, layer, last):
    if last:
        (ctx, hid, wo_hbm, out,
         wos, lhs, ys, yrecv, hl, pown, pfwd,
         wsem, csem, ysem, hsem, psem, fsem) = refs
    else:
        (ctx, x_hbm, wo_hbm, wq_hbm, wk_hbm, wv_hbm, kc_hbm, vc_hbm,
         q_out, kn_out, vn_out, hid_out, kb, vb,
         wos, lhs, ys, yrecv, hl, xs, wqs, wks, wvs, qacc, qown, qrecv,
         wsem, csem, ysem, hsem, qsem, kvsem) = refs
    rep, m, core, chip = place()
    across_m, mate_m = lax.rem(m + 2, 4), m + 1 - 2 * core
    across, mate = (rep, across_m), (rep, mate_m)
    rows = ctx.shape[1]
    chunks = hl.shape[0]
    load_wo = pltpu.make_async_copy(wo_hbm.at[layer], wos.at[core], wsem.at[0])
    load_wo.start()
    if not last:
        load_x = pltpu.make_async_copy(x_hbm.at[pl.ds(pl.multiple_of(m * rows, rows), rows)], xs, wsem.at[1])
        load_q = pltpu.make_async_copy(wq_hbm.at[layer + 1], wqs.at[core], wsem.at[2])
        load_k = pltpu.make_async_copy(wk_hbm.at[layer + 1], wks, wsem.at[3])
        load_v = pltpu.make_async_copy(wv_hbm.at[layer + 1], wvs, wsem.at[4])
        for c in (load_x, load_q, load_k, load_v):
            c.start()
    meet((across, mate))
    give = send(ctx.at[pl.ds((1 - chip) * 4, 4)], lhs.at[:, pl.ds(rows, rows), :], csem.at[0], csem.at[1], across)
    give.start()
    load_wo.wait()
    push_wo = send(wos.at[core], wos.at[core], wsem.at[5], wsem.at[6], mate)
    push_wo.start()
    if not last:
        load_q.wait()
        push_q = send(wqs.at[core], wqs.at[core], wsem.at[7], wsem.at[8], mate)
        push_q.start()
        caches = [pltpu.make_async_copy(kc_hbm.at[layer + 1], kb, kvsem.at[0]),
                  pltpu.make_async_copy(vc_hbm.at[layer + 1], vb, kvsem.at[1])]
        for c in caches:
            c.start()
    for i in range(4):
        lhs[i, 0:rows, :] = ctx[chip * 4 + i]
    give.wait()
    push_wo.wait()
    ycopies = []
    for j in range(chunks):
        y = dot(lhs[0], wos[0, 0:256, j * 256:(j + 1) * 256])
        for i in range(1, 4):
            y += dot(lhs[i], wos[i // 2, (i % 2) * 256:(i % 2 + 1) * 256, j * 256:(j + 1) * 256])
        ys[j] = y
        c = send(ys.at[j, pl.ds(rows, rows)], yrecv.at[j], ysem.at[0, j], ysem.at[1, j], across)
        c.start()
        ycopies.append(c)
    if not last:
        load_x.wait()
    hcopies = []
    pcopies = []
    for j in range(chunks):
        ycopies[j].wait_recv()
        old = hid[j] if last else xs[:, j * 256:(j + 1) * 256]
        new = (old.astype(F32) + (ys[j, 0:rows, :] + yrecv[j])).astype(BF16)
        hl[j, 0:rows, :] = new
        c = send(hl.at[j, pl.ds(0, rows)], hl.at[j, pl.ds(rows, rows)], hsem.at[0, j], hsem.at[1, j], across)
        c.start()
        hcopies.append(c)
        if last:
            c = send(hl.at[j, pl.ds(0, rows)], pown.at[j], psem.at[0, j], psem.at[1, j], mate)
            c.start()
            pcopies.append(c)
    if last:
        fcopies = []
        for j in range(chunks):
            hcopies[j].wait_recv()
            c = send(hl.at[j, pl.ds(rows, rows)], pfwd.at[j], fsem.at[0, j], fsem.at[1, j], mate)
            c.start()
            fcopies.append(c)
        for j in range(chunks):
            cols = slice(j * 256, (j + 1) * 256)
            out[pl.ds(pl.multiple_of(m * rows, rows), rows), cols] = hl[j, 0:rows, :]
            out[pl.ds(pl.multiple_of(across_m * rows, rows), rows), cols] = hl[j, rows:2 * rows, :]
        for j in range(chunks):
            cols = slice(j * 256, (j + 1) * 256)
            pcopies[j].wait_recv()
            out[pl.ds(pl.multiple_of(mate_m * rows, rows), rows), cols] = pown[j]
            fcopies[j].wait_recv()
            out[pl.ds(pl.multiple_of((3 - m) * rows, rows), rows), cols] = pfwd[j]
        for c in ycopies + hcopies + pcopies + fcopies:
            c.wait_send()
        return
    push_q.wait()
    for j in range(chunks):
        hcopies[j].wait_recv()
        for i in range(4):
            part = dot(hl[j], wqs[i // 2, j * 256:(j + 1) * 256, (i % 2) * 256:(i % 2 + 1) * 256])
            if j == 0:
                qacc[i] = part
            else:
                qacc[i] += part
    qcopies = []
    for i in range(4):
        qown[i] = qacc[i].astype(BF16)
        c = send(qown.at[i, pl.ds(rows, rows)], qrecv.at[i], qsem.at[0, i], qsem.at[1, i], across)
        c.start()
        qcopies.append(c)
    for load, w, res in ((load_k, wks, kn_out), (load_v, wvs, vn_out)):
        load.wait()
        t = dot(hl[0, 0:rows, :], w[0:256, :])
        for j in range(1, chunks):
            t += dot(hl[j, 0:rows, :], w[j * 256:(j + 1) * 256, :])
        res[...] = t.astype(BF16).astype(F32)
    for j in range(chunks):
        hid_out[j] = hl[j, 0:rows, :]
    for i in range(4):
        q_out[chip * 4 + i] = qown[i, 0:rows, :]
    for i in range(4):
        qcopies[i].wait_recv()
        q_out[(1 - chip) * 4 + i] = qrecv[i]
    for c in ycopies + hcopies + qcopies:
        c.wait_send()
    for c in caches:
        c.wait()


def solution(mesh):
    groups = mesh.shape["model"]
    row_axes = ("replica", "model")
    cache_spec = P(None, row_axes, None, None)

    def device_step(x, cache_len, w_query, w_key, w_value, w_out, k_cache, v_cache):
        layers, rows, seq, dim = k_cache.shape
        total, width = x.shape
        chunks = width // dim
        heads = w_query.shape[-1] // dim * groups
        local = w_query.shape[-1]
        hd = (heads, rows, dim)
        x, w_query, w_key, w_value, w_out, k_cache, v_cache = (
            pltpu.with_memory_space_constraint(a, pltpu.HBM)
            for a in (x, w_query, w_key, w_value, w_out, k_cache, v_cache))
        remote = functools.partial(pltpu.CompilerParams, has_side_effects=True)

        q, kn, vn, kb, vb = pl.pallas_call(
            first_kernel,
            out_shape=(pltpu.VMEM(hd, BF16), pltpu.VMEM((rows, dim), F32), pltpu.VMEM((rows, dim), F32),
                       pltpu.VMEM((rows, seq, dim), BF16), pltpu.VMEM((rows, seq, dim), BF16)),
            in_specs=[HBM] * 6,
            out_specs=(VM,) * 5,
            scratch_shapes=[
                pltpu.VMEM((total, width), BF16), pltpu.VMEM((2, width, dim), BF16),
                pltpu.VMEM((width, dim), BF16), pltpu.VMEM((width, dim), BF16),
                pltpu.VMEM((4, 2, rows, dim), BF16), pltpu.VMEM((4, 2, rows, dim), BF16),
                DMA((5,)), DMA((2,)), DMA((3, 2)), DMA((3, 2)),
            ],
            compiler_params=remote(collective_id=0, vmem_limit_bytes=16 << 20),
            name="first",
        )(x, w_query, w_key, w_value, k_cache, v_cache)

        ko = vo = None
        hid = x
        for layer in range(layers):
            last = layer == layers - 1
            ins = (cache_len, q, kn, vn, kb, vb) + ((ko, vo) if layer else ())
            ctx, _, _, ko, vo = pl.pallas_call(
                functools.partial(attend_kernel, layer=layer),
                out_shape=(pltpu.VMEM(hd, BF16), pltpu.VMEM(kb.shape, BF16), pltpu.VMEM(vb.shape, BF16),
                           jax.ShapeDtypeStruct(k_cache.shape, BF16), jax.ShapeDtypeStruct(v_cache.shape, BF16)),
                in_specs=[SM] + [VM] * 5 + ([HBM, HBM] if layer else []),
                out_specs=(VM, VM, VM, HBM, HBM),
                input_output_aliases={4: 1, 5: 2, 6: 3, 7: 4} if layer else {4: 1, 5: 2},
                scratch_shapes=[
                    pltpu.VMEM((dim // 128, rows * heads, 128), F32), pltpu.VMEM((rows * heads, seq), F32), DMA((2, rows // 16)),
                ],
                compiler_params=pltpu.CompilerParams(vmem_limit_bytes=8 << 20),
                name=f"attend{layer}",
            )(*ins)
            common = [
                pltpu.VMEM((2, local, width), BF16), pltpu.VMEM((4, 2 * rows, dim), BF16),
                pltpu.VMEM((chunks, 2 * rows, dim), F32), pltpu.VMEM((chunks, rows, dim), F32),
                pltpu.VMEM((chunks, 2 * rows, dim), BF16),
            ]
            sems = [DMA((9,)), DMA((2,)), DMA((2, chunks)), DMA((2, chunks))]
            if last:
                out = pl.pallas_call(
                    functools.partial(exchange_kernel, layer=layer, last=True),
                    out_shape=pltpu.VMEM((total, width), BF16),
                    in_specs=[VM, VM, HBM],
                    out_specs=VM,
                    scratch_shapes=common + [pltpu.VMEM((chunks, rows, dim), BF16)] * 2
                    + sems + [DMA((2, chunks)), DMA((2, chunks))],
                    compiler_params=remote(collective_id=layer + 1, vmem_limit_bytes=16 << 20),
                    name="last",
                )(ctx, hid, w_out)
            else:
                q, kn, vn, hid, kb, vb = pl.pallas_call(
                    functools.partial(exchange_kernel, layer=layer, last=False),
                    out_shape=(pltpu.VMEM(hd, BF16), pltpu.VMEM((rows, dim), F32), pltpu.VMEM((rows, dim), F32),
                               pltpu.VMEM((chunks, rows, dim), BF16),
                               pltpu.VMEM((rows, seq, dim), BF16), pltpu.VMEM((rows, seq, dim), BF16)),
                    in_specs=[VM] + [HBM] * 7,
                    out_specs=(VM,) * 6,
                    scratch_shapes=common + [
                        pltpu.VMEM((rows, width), BF16), pltpu.VMEM((2, width, local), BF16),
                        pltpu.VMEM((width, dim), BF16), pltpu.VMEM((width, dim), BF16),
                        pltpu.VMEM((4, 2 * rows, dim), F32), pltpu.VMEM((4, 2 * rows, dim), BF16),
                        pltpu.VMEM((4, rows, dim), BF16),
                    ] + sems + [DMA((2, 4)), DMA((2,))],
                    compiler_params=remote(collective_id=layer + 1, vmem_limit_bytes=24 << 20),
                    name="middle",
                )(ctx, hid, w_out, w_query, w_key, w_value, k_cache, v_cache)
        return out, ko, vo

    return jax.shard_map(
        device_step,
        mesh=mesh,
        in_specs=(P("replica", None), P("replica"), P(None, None, "model"), P(), P(), P(None, "model", None), cache_spec, cache_spec),
        out_specs=(P("replica", None), cache_spec, cache_spec),
        check_vma=False,
    )
```

```python
import functools

import jax
import jax.numpy as jnp
from jax import lax
from jax.experimental import pallas as pl
from jax.experimental.pallas import tpu as pltpu
from jax.sharding import PartitionSpec as P

F32 = jnp.float32
BF16 = jnp.bfloat16
MESH = pl.DeviceIdType.MESH
HBM = pl.BlockSpec(memory_space=pltpu.HBM)
VM = pl.BlockSpec(memory_space=pltpu.VMEM)
SM = pl.BlockSpec(memory_space=pltpu.SMEM)
DMA = pltpu.SemaphoreType.DMA


def dot(a, b):
    return jnp.dot(a, b, preferred_element_type=F32)


def place():
    m = lax.axis_index("model")
    return lax.axis_index("replica"), m, lax.rem(m, 2), m // 2


def meet(peers):
    barrier = pltpu.get_barrier_semaphore()
    for peer in peers:
        pl.semaphore_signal(barrier, inc=1, device_id=peer, device_id_type=MESH)
    pl.semaphore_wait(barrier, len(peers))


def send(src, dst, send_sem, recv_sem, peer):
    return pltpu.make_async_remote_copy(
        src_ref=src, dst_ref=dst, send_sem=send_sem, recv_sem=recv_sem, device_id=peer, device_id_type=MESH)


def scatter_queries(get, qs, heads, rows):
    for h in range(heads):
        for i in range(2):
            qs[i, pl.ds(h, rows, stride=heads), :] = get(h)[:, i * 128:(i + 1) * 128].astype(F32)


def attend_rows(which, heads, length, kb, vb, qs, st, new=None):
    seq, dim = kb.shape[1:]
    scale = dim ** -0.5
    pos = lax.broadcasted_iota(jnp.int32, (heads, seq), 1)
    for b in which:
        cut = slice(b * heads, (b + 1) * heads)
        q = jnp.concatenate([qs[i, cut, :] for i in range(2)], axis=1)
        s = lax.dot_general(q.astype(BF16), kb[b], (((1,), (1,)), ((), ())), preferred_element_type=F32)
        if new is not None:
            s = jnp.where(pos == length(b), jnp.sum(q * new[0][b:b + 1, :], axis=1, keepdims=True), s)
        s = jnp.where(pos <= length(b), s * scale, -jnp.inf)
        for i in range(2):
            st[4 * i + b // 8, b % 8 * heads:(b % 8 + 1) * heads, :] = s[:, i * 256:(i + 1) * 256]
    for b in which:
        cut = slice(b * heads, (b + 1) * heads)
        s = jnp.concatenate([st[4 * i + b // 8, b % 8 * heads:(b % 8 + 1) * heads, :] for i in range(2)], axis=1)
        e = jnp.exp(s - jnp.max(s, axis=1, keepdims=True))
        p = (e * (1.0 / jnp.sum(e, axis=1, keepdims=True))).astype(BF16)
        if new is None:
            c = dot(p, vb[b])
        else:
            here = pos == length(b)
            p = p.astype(F32)
            mine = jnp.sum(jnp.where(here, p, 0.0), axis=1, keepdims=True)
            c = dot(jnp.where(here, 0.0, p).astype(BF16), vb[b]) + mine * new[1][b:b + 1, :]
        for i in range(2):
            qs[i, cut, :] = c[:, i * 128:(i + 1) * 128]


def gather_contexts(ctx, qs, first, count, heads):
    for h in range(heads):
        for i in range(2):
            ctx[h, first:first + count, i * 128:(i + 1) * 128] = (
                qs[i, pl.ds(first * heads + h, count, stride=heads), :].astype(BF16))


def layer0_kernel(len_ref, x_hbm, wq_hbm, wk_hbm, wv_hbm, wo_hbm, kc_hbm, vc_hbm,
                  q_out, kvn, hl, wof, k0, v0, k1, v1,
                  xs, qown, qrecv, qs, ctx, wos, lhs, ys, yrecv, wq1, qacc, q1own, q1recv, stage,
                  wsem, lsem, csem, qsem, gsem, psem, ysem, hsem, q1sem, xsem, yzsem, msem):
    rep, m, core, chip = place()
    heads, rows, dim = q_out.shape
    half = rows // 2
    chunks = hl.shape[0]
    across_m, mate_m, diag_m = lax.rem(m + 2, 4), m + 1 - 2 * core, 3 - m
    across, mate, diag = (rep, across_m), (rep, mate_m), (rep, diag_m)
    rep_y, rep_z, rep_yz = rep + 1 - 2 * lax.rem(rep, 2), lax.rem(rep + 2, 4), 3 - rep
    next_y, next_z = (rep_y, m), (rep_z, m)
    span = wof.shape[2]
    quarter = stage.shape[0]
    sub = quarter // 2

    def piece(owner, r, s):
        start = pl.multiple_of(lax.rem(r, 2) * quarter + s * sub, sub)
        return wof.at[2 * owner + r // 2, pl.ds(start, sub), :]

    load_x = pltpu.make_async_copy(x_hbm, xs, wsem.at[0])
    load_x.start()
    deep = k1.shape[1]
    blocks = xs.shape[1] // deep
    loads = []
    for n, src in enumerate((wq_hbm.at[0, :, pl.ds(0, dim)], wq_hbm.at[0, :, pl.ds(dim, dim)], wk_hbm.at[0], wv_hbm.at[0])):
        loads.append([pltpu.make_async_copy(src.at[pl.ds(t * deep, deep)], k1.at[n * blocks + t], lsem.at[n, t])
                      for t in range(blocks)])
        for c in loads[n]:
            c.start()

    def first_weights(n, rows_ref):
        total = None
        for t in range(blocks):
            loads[n][t].wait()
            part = dot(rows_ref[:, t * deep:(t + 1) * deep], k1[n * blocks + t])
            total = part if t == 0 else total + part
        return total.astype(BF16)

    theirs = pl.ds(pl.multiple_of((1 - chip) * span, span), span)
    ours = pl.ds(pl.multiple_of(chip * span, span), span)
    load_stage = pltpu.make_async_copy(
        wo_hbm.at[1, pl.ds(pl.multiple_of(rep * quarter, quarter), quarter), theirs], stage, wsem.at[5])
    load_stage.start()
    meet((across, diag, mate, next_y, next_z))
    load_x.wait()
    qcopies = []
    for i in range(2):
        q = first_weights(i, xs)
        for d in range(4):
            qown[d, i] = q[d * rows:(d + 1) * rows]
        for n, (peer, who) in enumerate(((across, across_m), (diag, diag_m), (mate, mate_m))):
            c = send(qown.at[who, i], qrecv.at[m, i], qsem.at[0, n, i], qsem.at[1, n, i], peer)
            c.start()
            qcopies.append(c)
        qrecv[m, i] = qown[m, i]
    loads0 = [pltpu.make_async_copy(kc_hbm.at[0], k0, csem.at[0]), pltpu.make_async_copy(vc_hbm.at[0], v0, csem.at[1])]
    load_wo = pltpu.make_async_copy(wo_hbm.at[0], wos.at[core], wsem.at[6])
    load_q1 = pltpu.make_async_copy(wq_hbm.at[1], wq1.at[core], wsem.at[7])
    load_own = [pltpu.make_async_copy(wo_hbm.at[1, pl.ds(i * dim, dim), ours], wof.at[2 * m + i], wsem.at[8 + i])
                for i in range(2)]
    for c in loads0 + [load_wo, load_q1] + load_own:
        c.start()
    load_stage.wait()
    xcopies = []
    for s in range(2):
        c = send(stage.at[pl.ds(s * sub, sub)], piece(m, rep, s), xsem.at[0, s], xsem.at[1, s], across)
        c.start()
        xcopies.append(c)
    mine = xs[pl.ds(pl.multiple_of(m * rows, rows), rows), :]
    kvn[0] = first_weights(2, mine).astype(F32)
    kvn[1] = first_weights(3, mine).astype(F32)
    for c in qcopies:
        c.wait()
    scatter_queries(lambda h: qrecv[h // 2, h % 2], qs, heads, rows)
    loads0[0].wait()
    loads0[1].wait()
    loads1 = [pltpu.make_async_copy(kc_hbm.at[1], k1, csem.at[2]), pltpu.make_async_copy(vc_hbm.at[1], v1, csem.at[3])]
    for c in loads1:
        c.start()
    base = m * rows
    load_wo.wait()
    push_wo = send(wos.at[core], wos.at[core], psem.at[0, 0], psem.at[1, 0], mate)
    push_wo.start()
    load_q1.wait()
    push_q1 = send(wq1.at[core], wq1.at[core], psem.at[0, 1], psem.at[1, 1], mate)
    push_q1.start()
    gives = []
    for g in range(2):
        attend_rows(range(g * half, (g + 1) * half), heads, lambda b: len_ref[base + b], k0, v0, qs, ys, (kvn.at[0], kvn.at[1]))
        gather_contexts(ctx, qs, g * half, half, heads)
        c = send(ctx.at[pl.ds((1 - chip) * 4, 4), pl.ds(g * half, half), :],
                 lhs.at[:, pl.ds(rows + g * half, half), :], gsem.at[0, g], gsem.at[1, g], across)
        c.start()
        gives.append(c)
    for i in range(4):
        lhs[i, 0:rows, :] = ctx[chip * 4 + i]
    mcopies = []

    def to_mate(ref):
        n = len(mcopies)
        c = send(ref, ref, msem.at[0, n], msem.at[1, n], mate)
        c.start()
        mcopies.append(c)

    around = []
    for s in range(2):
        xcopies[s].wait_recv()
        for n, peer in enumerate((next_y, next_z)):
            ref = piece(across_m, rep, s)
            c = send(ref, ref, yzsem.at[0, n, s], yzsem.at[1, n, s], peer)
            c.start()
            around.append(c)
    push_wo.wait()
    for c in gives:
        c.wait()
    ycopies = []
    for j in range(chunks):
        y = dot(lhs[0], wos[0, 0:256, j * 256:(j + 1) * 256])
        for i in range(1, 4):
            y += dot(lhs[i], wos[i // 2, (i % 2) * 256:(i % 2 + 1) * 256, j * 256:(j + 1) * 256])
        ys[j] = y
        c = send(ys.at[j, pl.ds(rows, rows)], yrecv.at[j], ysem.at[0, j], ysem.at[1, j], across)
        c.start()
        ycopies.append(c)
    loads_kv = [[pltpu.make_async_copy(src.at[1, pl.ds(j * dim, dim)], wos.at[0, pl.ds(n * dim, dim), pl.ds(j * dim, dim)],
                                       lsem.at[4 + n, j]) for j in range(chunks)] for n, src in enumerate((wk_hbm, wv_hbm))]
    for c in loads_kv[0] + loads_kv[1]:
        c.start()
    for i in range(2):
        load_own[i].wait()
        to_mate(wof.at[2 * m + i])
    for s in range(2):
        to_mate(piece(across_m, rep, s))
    hcopies = []
    for j in range(chunks):
        ycopies[j].wait_recv()
        old = xs[pl.ds(pl.multiple_of(m * rows, rows), rows), j * 256:(j + 1) * 256]
        hl[j, 0:rows, :] = (old.astype(F32) + (ys[j, 0:rows, :] + yrecv[j])).astype(BF16)
        c = send(hl.at[j, pl.ds(0, rows)], hl.at[j, pl.ds(rows, rows)], hsem.at[0, j], hsem.at[1, j], across)
        c.start()
        hcopies.append(c)
    for c in around:
        c.wait_recv()
    for s, (n, peer, other) in enumerate(((1, next_z, rep_y), (0, next_y, rep_z))):
        ref = piece(across_m, other, s)
        c = send(ref, ref, yzsem.at[0, n, 2], yzsem.at[1, n, 2], peer)
        c.start()
        around.append(c)
    for other in (rep_y, rep_z):
        for s in range(2):
            to_mate(piece(across_m, other, s))
    push_q1.wait()
    for j in range(chunks):
        hcopies[j].wait_recv()
        for i in range(4):
            part = dot(hl[j], wq1[i // 2, j * 256:(j + 1) * 256, (i % 2) * 256:(i % 2 + 1) * 256])
            if j == 0:
                qacc[i] = part
            else:
                qacc[i] += part
    q1copies = []
    for i in range(4):
        q1own[i] = qacc[i].astype(BF16)
        c = send(q1own.at[i, pl.ds(rows, rows)], q1recv.at[i], q1sem.at[0, i], q1sem.at[1, i], across)
        c.start()
        q1copies.append(c)
    for n in range(2):
        for j in range(chunks):
            loads_kv[n][j].wait()
            part = dot(hl[j, 0:rows, :], wos[0, n * dim:(n + 1) * dim, j * dim:(j + 1) * dim])
            t = part if j == 0 else t + part
        kvn[2 + n] = t.astype(BF16).astype(F32)
    for i in range(4):
        q_out[chip * 4 + i] = q1own[i, 0:rows, :]
    for s in range(2):
        around[4 + s].wait_recv()
    for s in range(2):
        to_mate(piece(across_m, rep_yz, s))
    for i in range(4):
        q1copies[i].wait_recv()
        q_out[(1 - chip) * 4 + i] = q1recv[i]
    for c in mcopies:
        c.wait()
    for c in xcopies + around + ycopies + hcopies + q1copies:
        c.wait_send()
    for c in loads1:
        c.wait()


def attend1_kernel(len_ref, q_ref, kvn, k0, v0, k1, v1, ctx, _k0, _v0, _k1, _v1, ko, vo, qs, st, osem):
    heads, rows, dim = q_ref.shape
    base = lax.axis_index("model") * rows
    tile = 16
    outs = []
    for layer, bufs in enumerate(((k0, v0), (k1, v1))):
        def patch(b, carry):
            ln = len_ref[base + b]
            start = pl.multiple_of((ln // tile) * tile, tile)
            hit = lax.broadcasted_iota(jnp.int32, (tile, dim), 0) == ln - start
            for n, buf in enumerate(bufs):
                old = buf[b, pl.ds(start, tile), :].astype(F32)
                buf[b, pl.ds(start, tile), :] = jnp.where(hit, kvn[2 * layer + n, pl.ds(b, 1), :], old).astype(BF16)
            return carry

        lax.fori_loop(0, rows, patch, 0, unroll=4)
        for i in range(2):
            for n, (src, dst) in enumerate(zip(bufs, (ko, vo))):
                part = pl.ds(i * (rows // 2), rows // 2)
                c = pltpu.make_async_copy(src.at[part], dst.at[layer, part], osem.at[layer, n, i])
                c.start()
                outs.append(c)
    scatter_queries(lambda h: q_ref[h], qs, heads, rows)
    attend_rows(range(rows), heads, lambda b: len_ref[base + b], k1, v1, qs, st)
    gather_contexts(ctx, qs, 0, rows, heads)
    for c in outs:
        c.wait()


def last_kernel(ctx, hid, wof, out, other, acc, hl, pl2, gsem, hsem, psem):
    rep, m, core, chip = place()
    across_m, mate_m = lax.rem(m + 2, 4), m + 1 - 2 * core
    across, mate = (rep, across_m), (rep, mate_m)
    heads, rows, dim = ctx.shape
    chunks = hl.shape[0]
    cols = chunks // 2
    meet((across, mate))
    gives = []
    for p in range(4):
        two = pl.ds(2 * p, 2)
        c = send(ctx.at[two], other.at[two], gsem.at[0, p], gsem.at[1, p], across)
        c.start()
        gives.append(c)
    hcopies = []
    pcopies = []

    def to_mate(at):
        n = len(pcopies)
        c = send(hl.at[at], pl2.at[at], psem.at[0, n], psem.at[1, n], mate)
        c.start()
        pcopies.append(c)

    for p in range(4):
        gives[p].wait_recv()
        left = [jnp.concatenate((ctx[2 * p + i], other[2 * p + i]), axis=0) for i in range(2)]
        for j in range(cols):
            part = dot(left[0], wof[2 * p, :, j * dim:(j + 1) * dim]) + dot(left[1], wof[2 * p + 1, :, j * dim:(j + 1) * dim])
            if p == 0:
                acc[j] = part
            elif p < 3:
                acc[j] += part
            else:
                at = chip * cols + j
                hl[at] = (hid[at].astype(F32) + (acc[j] + part)).astype(BF16)
                for n in range(2):
                    c = send(hl.at[at, pl.ds(n * rows, rows)], hl.at[at, pl.ds((1 - n) * rows, rows)],
                             hsem.at[0, n, j], hsem.at[1, n, j], across)
                    c.start()
                    hcopies.append(c)
                to_mate(at)
    for j in range(cols):
        for n in range(2):
            hcopies[2 * j + n].wait_recv()
        to_mate((1 - chip) * cols + j)

    def put(who, at, value):
        out[pl.ds(pl.multiple_of(who * rows, rows), rows), at * dim:(at + 1) * dim] = value

    for j in range(chunks):
        put(m, j, hl[j, 0:rows, :])
        put(across_m, j, hl[j, rows:2 * rows, :])
    for c in pcopies:
        c.wait_recv()
    for j in range(chunks):
        put(mate_m, j, pl2[j, 0:rows, :])
        put(3 - m, j, pl2[j, rows:2 * rows, :])
    for c in gives + hcopies + pcopies:
        c.wait_send()


def solution(mesh):
    row_axes = ("replica", "model")
    cache_spec = P(None, row_axes, None, None)

    def device_step(x, cache_len, w_query, w_key, w_value, w_out, k_cache, v_cache):
        layers, rows, seq, dim = k_cache.shape
        total, width = x.shape
        chunks = width // dim
        local = w_query.shape[-1]
        heads = local // dim * mesh.shape["model"]
        hd = (heads, rows, dim)
        x, w_query, w_key, w_value, w_out, k_cache, v_cache = (
            pltpu.with_memory_space_constraint(a, pltpu.HBM)
            for a in (x, w_query, w_key, w_value, w_out, k_cache, v_cache))
        remote = functools.partial(pltpu.CompilerParams, has_side_effects=True)
        cache = pltpu.VMEM((rows, seq, dim), BF16)
        qs = pltpu.VMEM((2, rows * heads, 128), F32)
        st = pltpu.VMEM((chunks, 2 * rows, dim), F32)

        q, kvn, hid, wof, *caches = pl.pallas_call(
            layer0_kernel,
            out_shape=(pltpu.VMEM(hd, BF16), pltpu.VMEM((4, rows, dim), F32), pltpu.VMEM((chunks, 2 * rows, dim), BF16),
                       pltpu.VMEM((heads, dim, width // 2), BF16)) + (cache,) * 4,
            in_specs=[SM] + [HBM] * 7,
            out_specs=(VM,) * 8,
            scratch_shapes=[
                pltpu.VMEM((total, width), BF16),
                pltpu.VMEM((4, 2, rows, dim), BF16), pltpu.VMEM((4, 2, rows, dim), BF16),
                qs, pltpu.VMEM(hd, BF16),
                pltpu.VMEM((2, local, width), BF16), pltpu.VMEM((4, 2 * rows, dim), BF16),
                pltpu.VMEM((chunks, 2 * rows, dim), F32), pltpu.VMEM((chunks, rows, dim), F32),
                pltpu.VMEM((2, width, local), BF16),
                pltpu.VMEM((4, 2 * rows, dim), F32), pltpu.VMEM((4, 2 * rows, dim), BF16),
                pltpu.VMEM((4, rows, dim), BF16), pltpu.VMEM((local // 4, width // 2), BF16),
                DMA((10,)), DMA((6, 8)), DMA((4,)), DMA((2, 3, 2)), DMA((2, 2)), DMA((2, 2)), DMA((2, chunks)), DMA((2, chunks)),
                DMA((2, 4)), DMA((2, 2)), DMA((2, 2, 3)), DMA((2, 10)),
            ],
            compiler_params=remote(collective_id=0, vmem_limit_bytes=11 << 20),
            name="layer0",
        )(cache_len, x, w_query, w_key, w_value, w_out, k_cache, v_cache)

        ctx, _, _, _, _, ko, vo = pl.pallas_call(
            attend1_kernel,
            out_shape=(pltpu.VMEM(hd, BF16), cache, cache, cache, cache,
                       jax.ShapeDtypeStruct(k_cache.shape, BF16), jax.ShapeDtypeStruct(v_cache.shape, BF16)),
            in_specs=[SM] + [VM] * 6,
            out_specs=(VM,) * 5 + (HBM, HBM),
            input_output_aliases={3: 1, 4: 2, 5: 3, 6: 4},
            scratch_shapes=[qs, st, DMA((2, 2, 2))],
            compiler_params=pltpu.CompilerParams(vmem_limit_bytes=3 << 20),
            name="attend1",
        )(cache_len, q, kvn, *caches)

        out = pl.pallas_call(
            last_kernel,
            out_shape=pltpu.VMEM((total, width), BF16),
            in_specs=[VM] * 3,
            out_specs=VM,
            scratch_shapes=[
                pltpu.VMEM(hd, BF16), pltpu.VMEM((chunks // 2, 2 * rows, dim), F32),
                pltpu.VMEM((chunks, 2 * rows, dim), BF16), pltpu.VMEM((chunks, 2 * rows, dim), BF16),
                DMA((2, 4)), DMA((2, 2, chunks // 2)), DMA((2, chunks)),
            ],
            compiler_params=remote(collective_id=1, vmem_limit_bytes=4 << 20),
            name="last",
        )(ctx, hid, wof)
        return out, ko, vo

    return jax.shard_map(
        device_step,
        mesh=mesh,
        in_specs=(P("replica", None), P("replica"), P(None, None, "model"), P(), P(), P(None, "model", None), cache_spec, cache_spec),
        out_specs=(P("replica", None), cache_spec, cache_spec),
        check_vma=False,
    )
```

```python
import functools

import jax
import jax.numpy as jnp
from jax import lax
from jax.experimental import pallas as pl
from jax.experimental.pallas import tpu as pltpu
from jax.sharding import PartitionSpec as P

F32 = jnp.float32
BF16 = jnp.bfloat16
MESH = pl.DeviceIdType.MESH
HBM = pl.BlockSpec(memory_space=pltpu.HBM)
VM = pl.BlockSpec(memory_space=pltpu.VMEM)
SM = pl.BlockSpec(memory_space=pltpu.SMEM)
DMA = pltpu.SemaphoreType.DMA


def dot(a, b):
    return jnp.dot(a, b, preferred_element_type=F32)


def place():
    m = lax.axis_index("model")
    return lax.axis_index("replica"), m, lax.rem(m, 2), m // 2


def greet(peers):
    barrier = pltpu.get_barrier_semaphore()
    for peer in peers:
        pl.semaphore_signal(barrier, inc=1, device_id=peer, device_id_type=MESH)


def meet(peers):
    pl.semaphore_wait(pltpu.get_barrier_semaphore(), len(peers))


def send(src, dst, send_sem, recv_sem, peer):
    return pltpu.make_async_remote_copy(
        src_ref=src, dst_ref=dst, send_sem=send_sem, recv_sem=recv_sem, device_id=peer, device_id_type=MESH)


def scatter_queries(get, qs, heads, rows):
    for h in range(heads):
        for i in range(2):
            qs[i, pl.ds(h, rows, stride=heads), :] = get(h)[:, i * 128:(i + 1) * 128].astype(F32)


def attend_rows(which, heads, length, kb, vb, qs, st, new=None, values=None):
    seq, dim = kb.shape[1:]
    scale = dim ** -0.5
    pos = lax.broadcasted_iota(jnp.int32, (heads, seq), 1)
    for b in which:
        cut = slice(b * heads, (b + 1) * heads)
        q = jnp.concatenate([qs[i, cut, :] for i in range(2)], axis=1)
        s = lax.dot_general(q.astype(BF16), kb[b], (((1,), (1,)), ((), ())), preferred_element_type=F32)
        if new is not None:
            s = jnp.where(pos == length(b), jnp.sum(q * new[0][b:b + 1, :], axis=1, keepdims=True), s)
        s = jnp.where(pos <= length(b), s * scale, -jnp.inf)
        for i in range(2):
            st[4 * i + b // 8, b % 8 * heads:(b % 8 + 1) * heads, :] = s[:, i * 256:(i + 1) * 256]
    if values is not None:
        values.wait()
    for b in which:
        cut = slice(b * heads, (b + 1) * heads)
        s = jnp.concatenate([st[4 * i + b // 8, b % 8 * heads:(b % 8 + 1) * heads, :] for i in range(2)], axis=1)
        e = jnp.exp(s - jnp.max(s, axis=1, keepdims=True))
        p = (e * (1.0 / jnp.sum(e, axis=1, keepdims=True))).astype(BF16)
        if new is None:
            c = dot(p, vb[b])
        else:
            here = pos == length(b)
            p = p.astype(F32)
            mine = jnp.sum(jnp.where(here, p, 0.0), axis=1, keepdims=True)
            c = dot(jnp.where(here, 0.0, p).astype(BF16), vb[b]) + mine * new[1][b:b + 1, :]
        for i in range(2):
            qs[i, cut, :] = c[:, i * 128:(i + 1) * 128]


def gather_contexts(ctx, qs, first, count, heads):
    for h in range(heads):
        for i in range(2):
            ctx[h, first:first + count, i * 128:(i + 1) * 128] = (
                qs[i, pl.ds(first * heads + h, count, stride=heads), :].astype(BF16))


def layer0_kernel(len_ref, x_hbm, wq_hbm, wk_hbm, wv_hbm, wo_hbm, kc_hbm, vc_hbm,
                  q_out, kvn, hl, wof, k0, v0, k1, v1,
                  xs, qown, qrecv, qs, ctx, wos, lhs, ys, yrecv, wq1, qacc, q1own, q1recv, stage,
                  wsem, lsem, csem, qsem, gsem, psem, ysem, hsem, q1sem, xsem, yzsem, msem):
    rep, m, core, chip = place()
    heads, rows, dim = q_out.shape
    half = rows // 2
    chunks = hl.shape[0]
    across_m, mate_m, diag_m = lax.rem(m + 2, 4), m + 1 - 2 * core, 3 - m
    across, mate, diag = (rep, across_m), (rep, mate_m), (rep, diag_m)
    rep_y, rep_z, rep_yz = rep + 1 - 2 * lax.rem(rep, 2), lax.rem(rep + 2, 4), 3 - rep
    next_y, next_z = (rep_y, m), (rep_z, m)
    span = wof.shape[2]
    quarter = stage.shape[0]
    subs = 4
    sub = quarter // subs

    def piece(owner, r, s):
        start = pl.multiple_of(lax.rem(r, 2) * quarter + s * sub, sub)
        return wof.at[2 * owner + r // 2, pl.ds(start, sub), :]

    friends = (across, diag, mate, next_y, next_z)
    greet(friends)
    xcopies = []

    def send_quarter(s):
        c = send(stage.at[pl.ds(s * sub, sub)], piece(m, rep, s), xsem.at[0, s], xsem.at[1, s], across)
        c.start()
        xcopies.append(c)

    around = []

    def pass_round(s):
        xcopies[s].wait_recv()
        ref = piece(across_m, rep, s)
        for n, peer in enumerate((next_y, next_z)):
            c = send(ref, ref, yzsem.at[0, n, s], yzsem.at[1, n, s], peer)
            c.start()
            around.append(c)

    load_x = pltpu.make_async_copy(x_hbm, xs, wsem.at[0])
    load_x.start()
    deep = k1.shape[1]
    blocks = xs.shape[1] // deep
    loads = []
    for n, src in enumerate((wq_hbm.at[0, :, pl.ds(0, dim)], wq_hbm.at[0, :, pl.ds(dim, dim)], wk_hbm.at[0], wv_hbm.at[0])):
        loads.append([pltpu.make_async_copy(src.at[pl.ds(t * deep, deep)], k1.at[n * blocks + t], lsem.at[n, t])
                      for t in range(blocks)])

    def start(copies):
        for c in copies:
            c.start()

    start(loads[0] + loads[1])

    def first_weights(n, rows_ref):
        total = None
        for t in range(blocks):
            loads[n][t].wait()
            part = dot(rows_ref[:, t * deep:(t + 1) * deep], k1[n * blocks + t])
            total = part if t == 0 else total + part
        return total.astype(BF16)

    theirs = pl.ds(pl.multiple_of((1 - chip) * span, span), span)
    ours = pl.ds(pl.multiple_of(chip * span, span), span)
    load_stage = pltpu.make_async_copy(
        wo_hbm.at[1, pl.ds(pl.multiple_of(rep * quarter, quarter), quarter), theirs], stage, wsem.at[5])
    load_stage.start()
    loads0 = [pltpu.make_async_copy(kc_hbm.at[0], k0, csem.at[0]), pltpu.make_async_copy(vc_hbm.at[0], v0, csem.at[1])]
    load_x.wait()
    start(loads[2] + loads[3])
    qcopies = []
    for i in range(2):
        q = first_weights(i, xs)
        if i == 0:
            start(loads0[:1])
            meet(friends)
            load_stage.wait()
        for d in range(4):
            qown[d, i] = q[d * rows:(d + 1) * rows]
        for n, (peer, who) in enumerate(((across, across_m), (diag, diag_m), (mate, mate_m))):
            c = send(qown.at[who, i], qrecv.at[m, i], qsem.at[0, n, i], qsem.at[1, n, i], peer)
            c.start()
            qcopies.append(c)
        qrecv[m, i] = qown[m, i]
    load_wo = pltpu.make_async_copy(wo_hbm.at[0], wos.at[core], wsem.at[6])
    load_q1 = pltpu.make_async_copy(wq_hbm.at[1], wq1.at[core], wsem.at[7])
    load_own = [pltpu.make_async_copy(wo_hbm.at[1, pl.ds(i * dim, dim), ours], wof.at[2 * m + i], wsem.at[8 + i])
                for i in range(2)]
    start(loads0[1:])
    for s in range(subs):
        send_quarter(s)
    mine = xs[pl.ds(pl.multiple_of(m * rows, rows), rows), :]
    kvn[0] = first_weights(2, mine).astype(F32)
    kvn[1] = first_weights(3, mine).astype(F32)
    for c in qcopies:
        c.wait()
    scatter_queries(lambda h: qrecv[h // 2, h % 2], qs, heads, rows)
    loads0[0].wait()
    start([load_wo, load_q1] + load_own)
    loads1 = [pltpu.make_async_copy(kc_hbm.at[1], k1, csem.at[2]), pltpu.make_async_copy(vc_hbm.at[1], v1, csem.at[3])]
    base = m * rows
    pass_round(0)
    gives = []
    for g in range(2):
        attend_rows(range(g * half, (g + 1) * half), heads, lambda b: len_ref[base + b], k0, v0, qs, ys,
                    (kvn.at[0], kvn.at[1]), loads0[1] if g == 0 else None)
        gather_contexts(ctx, qs, g * half, half, heads)
        c = send(ctx.at[pl.ds((1 - chip) * 4, 4), pl.ds(g * half, half), :],
                 lhs.at[:, pl.ds(rows + g * half, half), :], gsem.at[0, g], gsem.at[1, g], across)
        c.start()
        gives.append(c)
        if g == 0:
            start(loads1)
            load_wo.wait()
            push_wo = send(wos.at[core], wos.at[core], psem.at[0, 0], psem.at[1, 0], mate)
            push_wo.start()
            load_q1.wait()
            push_q1 = send(wq1.at[core], wq1.at[core], psem.at[0, 1], psem.at[1, 1], mate)
            push_q1.start()
            pass_round(1)
    for i in range(4):
        lhs[i, 0:rows, :] = ctx[chip * 4 + i]
    mcopies = []

    def to_mate(ref):
        n = len(mcopies)
        c = send(ref, ref, msem.at[0, n], msem.at[1, n], mate)
        c.start()
        mcopies.append(c)

    for s in range(2, subs):
        pass_round(s)
    push_wo.wait()
    for c in gives:
        c.wait()
    ycopies = []
    for j in range(chunks):
        y = dot(lhs[0], wos[0, 0:256, j * 256:(j + 1) * 256])
        for i in range(1, 4):
            y += dot(lhs[i], wos[i // 2, (i % 2) * 256:(i % 2 + 1) * 256, j * 256:(j + 1) * 256])
        ys[j] = y
        c = send(ys.at[j, pl.ds(rows, rows)], yrecv.at[j], ysem.at[0, j], ysem.at[1, j], across)
        c.start()
        ycopies.append(c)
    loads_kv = [[pltpu.make_async_copy(src.at[1, pl.ds(j * dim, dim)], wos.at[0, pl.ds(n * dim, dim), pl.ds(j * dim, dim)],
                                       lsem.at[4 + n, j]) for j in range(chunks)] for n, src in enumerate((wk_hbm, wv_hbm))]
    for c in loads_kv[0] + loads_kv[1]:
        c.start()
    for i in range(2):
        load_own[i].wait()
        to_mate(wof.at[2 * m + i])
    for s in range(subs):
        to_mate(piece(across_m, rep, s))
    for c in around:
        c.wait_recv()
    for s in range(subs):
        n, peer, other = ((1, next_z, rep_y), (0, next_y, rep_z))[s % 2]
        ref = piece(across_m, other, s)
        c = send(ref, ref, yzsem.at[0, n, subs + s // 2], yzsem.at[1, n, subs + s // 2], peer)
        c.start()
        around.append(c)
    for other in (rep_y, rep_z):
        for s in range(subs):
            to_mate(piece(across_m, other, s))
    hcopies = []
    for j in range(chunks):
        ycopies[j].wait_recv()
        old = xs[pl.ds(pl.multiple_of(m * rows, rows), rows), j * 256:(j + 1) * 256]
        hl[j, 0:rows, :] = (old.astype(F32) + (ys[j, 0:rows, :] + yrecv[j])).astype(BF16)
        c = send(hl.at[j, pl.ds(0, rows)], hl.at[j, pl.ds(rows, rows)], hsem.at[0, j], hsem.at[1, j], across)
        c.start()
        hcopies.append(c)
    push_q1.wait()
    for j in range(chunks):
        hcopies[j].wait_recv()
        for i in range(4):
            part = dot(hl[j], wq1[i // 2, j * 256:(j + 1) * 256, (i % 2) * 256:(i % 2 + 1) * 256])
            if j == 0:
                qacc[i] = part
            else:
                qacc[i] += part
    q1copies = []
    for i in range(4):
        q1own[i] = qacc[i].astype(BF16)
        c = send(q1own.at[i, pl.ds(rows, rows)], q1recv.at[i], q1sem.at[0, i], q1sem.at[1, i], across)
        c.start()
        q1copies.append(c)
    for n in range(2):
        for j in range(chunks):
            loads_kv[n][j].wait()
            part = dot(hl[j, 0:rows, :], wos[0, n * dim:(n + 1) * dim, j * dim:(j + 1) * dim])
            t = part if j == 0 else t + part
        kvn[2 + n] = t.astype(BF16).astype(F32)
    for i in range(4):
        q_out[chip * 4 + i] = q1own[i, 0:rows, :]
    for s in range(subs):
        around[2 * subs + s].wait_recv()
    for s in range(subs):
        to_mate(piece(across_m, rep_yz, s))
    for i in range(4):
        q1copies[i].wait_recv()
        q_out[(1 - chip) * 4 + i] = q1recv[i]
    for c in mcopies:
        c.wait()
    for c in xcopies + around + ycopies + hcopies + q1copies:
        c.wait_send()
    for c in loads1:
        c.wait()


def write_out(bufs, ko, vo, layer, sems):
    outs = []
    for i in range(2):
        for n, (src, dst) in enumerate(zip(bufs, (ko, vo))):
            part = pl.ds(i * (src.shape[0] // 2), src.shape[0] // 2)
            c = pltpu.make_async_copy(src.at[part], dst.at[layer, part], sems.at[n, i])
            c.start()
            outs.append(c)
    return outs


def write1_kernel(k1, v1, _k, _v, ko, vo, osem):
    for c in write_out((k1, v1), ko, vo, 1, osem):
        c.wait()


def attend1_kernel(len_ref, q_ref, kvn, k0, v0, k1, v1, ctx, _k0, _v0, _k1, _v1, ko, vo, qs, st, osem):
    heads, rows, dim = q_ref.shape
    base = lax.axis_index("model") * rows
    tile = 16
    for layer, bufs in enumerate(((k0, v0), (k1, v1))):
        def patch(b, carry):
            ln = len_ref[base + b]
            start = pl.multiple_of((ln // tile) * tile, tile)
            hit = lax.broadcasted_iota(jnp.int32, (tile, dim), 0) == ln - start
            for n, buf in enumerate(bufs):
                old = buf[b, pl.ds(start, tile), :].astype(F32)
                buf[b, pl.ds(start, tile), :] = jnp.where(hit, kvn[2 * layer + n, pl.ds(b, 1), :], old).astype(BF16)
            return carry

        lax.fori_loop(0, rows, patch, 0, unroll=4)
        if layer == 0:
            outs = write_out(bufs, ko, vo, 0, osem)
    scatter_queries(lambda h: q_ref[h], qs, heads, rows)
    attend_rows(range(rows), heads, lambda b: len_ref[base + b], k1, v1, qs, st)
    gather_contexts(ctx, qs, 0, rows, heads)
    for c in outs:
        c.wait()


def last_kernel(ctx, other, hid, wof, out, acc, hl, pl2, hsem, psem):
    rep, m, core, chip = place()
    across_m, mate_m = lax.rem(m + 2, 4), m + 1 - 2 * core
    across, mate = (rep, across_m), (rep, mate_m)
    heads, rows, dim = ctx.shape
    chunks = hl.shape[0]
    cols = chunks // 2
    greet((across, mate))
    hcopies = []
    pcopies = []

    def to_mate(at):
        n = len(pcopies)
        c = send(hl.at[at], pl2.at[at], psem.at[0, n], psem.at[1, n], mate)
        c.start()
        pcopies.append(c)

    for p in range(4):
        left = [jnp.concatenate((ctx[2 * p + i], other[2 * p + i]), axis=0) for i in range(2)]
        for j in range(cols):
            part = dot(left[0], wof[2 * p, :, j * dim:(j + 1) * dim]) + dot(left[1], wof[2 * p + 1, :, j * dim:(j + 1) * dim])
            if p == 0:
                acc[j] = part
            elif p < 3:
                acc[j] += part
            else:
                at = chip * cols + j
                if j == 0:
                    meet((across, mate))
                hl[at] = (hid[at].astype(F32) + (acc[j] + part)).astype(BF16)
                for n in range(2):
                    c = send(hl.at[at, pl.ds(n * rows, rows)], hl.at[at, pl.ds((1 - n) * rows, rows)],
                             hsem.at[0, n, j], hsem.at[1, n, j], across)
                    c.start()
                    hcopies.append(c)
                to_mate(at)
    for j in range(cols):
        for n in range(2):
            hcopies[2 * j + n].wait_recv()
        to_mate((1 - chip) * cols + j)

    def put(who, at, value):
        out[pl.ds(pl.multiple_of(who * rows, rows), rows), at * dim:(at + 1) * dim] = value

    for j in range(chunks):
        put(m, j, hl[j, 0:rows, :])
        put(across_m, j, hl[j, rows:2 * rows, :])
    for c in pcopies:
        c.wait_recv()
    for j in range(chunks):
        put(mate_m, j, pl2[j, 0:rows, :])
        put(3 - m, j, pl2[j, rows:2 * rows, :])
    for c in hcopies + pcopies:
        c.wait_send()


def solution(mesh):
    row_axes = ("replica", "model")
    cache_spec = P(None, row_axes, None, None)

    def device_step(x, cache_len, w_query, w_key, w_value, w_out, k_cache, v_cache):
        layers, rows, seq, dim = k_cache.shape
        total, width = x.shape
        chunks = width // dim
        local = w_query.shape[-1]
        heads = local // dim * mesh.shape["model"]
        hd = (heads, rows, dim)
        x, cache_len, w_query, w_key, w_value, w_out, k_cache, v_cache = (
            pltpu.with_memory_space_constraint(a, pltpu.HBM)
            for a in (x, cache_len, w_query, w_key, w_value, w_out, k_cache, v_cache))
        remote = functools.partial(pltpu.CompilerParams, has_side_effects=True)
        cache = pltpu.VMEM((rows, seq, dim), BF16)
        qs = pltpu.VMEM((2, rows * heads, 128), F32)
        st = pltpu.VMEM((chunks, 2 * rows, dim), F32)

        q, kvn, hid, wof, *caches = pl.pallas_call(
            layer0_kernel,
            out_shape=(pltpu.VMEM(hd, BF16), pltpu.VMEM((4, rows, dim), F32), pltpu.VMEM((chunks, 2 * rows, dim), BF16),
                       pltpu.VMEM((heads, dim, width // 2), BF16)) + (cache,) * 4,
            in_specs=[SM] + [HBM] * 7,
            out_specs=(VM,) * 8,
            scratch_shapes=[
                pltpu.VMEM((total, width), BF16),
                pltpu.VMEM((4, 2, rows, dim), BF16), pltpu.VMEM((4, 2, rows, dim), BF16),
                qs, pltpu.VMEM(hd, BF16),
                pltpu.VMEM((2, local, width), BF16), pltpu.VMEM((4, 2 * rows, dim), BF16),
                pltpu.VMEM((chunks, 2 * rows, dim), F32), pltpu.VMEM((chunks, rows, dim), F32),
                pltpu.VMEM((2, width, local), BF16),
                pltpu.VMEM((4, 2 * rows, dim), F32), pltpu.VMEM((4, 2 * rows, dim), BF16),
                pltpu.VMEM((4, rows, dim), BF16), pltpu.VMEM((local // 4, width // 2), BF16),
                DMA((10,)), DMA((6, 8)), DMA((4,)), DMA((2, 3, 2)), DMA((2, 2)), DMA((2, 2)), DMA((2, chunks)), DMA((2, chunks)),
                DMA((2, 4)), DMA((2, 4)), DMA((2, 2, 6)), DMA((2, 18)),
            ],
            compiler_params=remote(collective_id=0, vmem_limit_bytes=11 << 20),
            name="layer0",
        )(cache_len, x, w_query, w_key, w_value, w_out, k_cache, v_cache)

        ctx, _, _, k1, v1, ko, vo = pl.pallas_call(
            attend1_kernel,
            out_shape=(pltpu.VMEM(hd, BF16), cache, cache, cache, cache,
                       jax.ShapeDtypeStruct(k_cache.shape, BF16), jax.ShapeDtypeStruct(v_cache.shape, BF16)),
            in_specs=[SM] + [VM] * 6,
            out_specs=(VM,) * 5 + (HBM, HBM),
            input_output_aliases={3: 1, 4: 2, 5: 3, 6: 4},
            scratch_shapes=[qs, st, DMA((2, 2))],
            compiler_params=pltpu.CompilerParams(vmem_limit_bytes=3 << 20),
            name="attend1",
        )(cache_len, q, kvn, *caches)

        other = lax.ppermute(ctx, "model", [(i, (i + 2) % 4) for i in range(4)])
        ko, vo = pl.pallas_call(
            write1_kernel,
            out_shape=(jax.ShapeDtypeStruct(k_cache.shape, BF16), jax.ShapeDtypeStruct(v_cache.shape, BF16)),
            in_specs=[VM, VM, HBM, HBM],
            out_specs=(HBM, HBM),
            input_output_aliases={2: 0, 3: 1},
            scratch_shapes=[DMA((2, 2))],
            compiler_params=pltpu.CompilerParams(vmem_limit_bytes=1 << 20),
            cost_estimate=pl.CostEstimate(flops=10 ** 9, bytes_accessed=2 ** 25, transcendentals=0),
            name="write1",
        )(k1, v1, ko, vo)

        out = pl.pallas_call(
            last_kernel,
            out_shape=pltpu.VMEM((total, width), BF16),
            in_specs=[VM] * 4,
            out_specs=VM,
            scratch_shapes=[
                pltpu.VMEM((chunks // 2, 2 * rows, dim), F32),
                pltpu.VMEM((chunks, 2 * rows, dim), BF16), pltpu.VMEM((chunks, 2 * rows, dim), BF16),
                DMA((2, 2, chunks // 2)), DMA((2, chunks)),
            ],
            compiler_params=remote(collective_id=1, vmem_limit_bytes=4 << 20),
            name="last",
        )(ctx, other, hid, wof)
        return out, ko, vo

    return jax.shard_map(
        device_step,
        mesh=mesh,
        in_specs=(P("replica", None), P("replica"), P(None, None, "model"), P(), P(), P(None, "model", None), cache_spec, cache_spec),
        out_specs=(P("replica", None), cache_spec, cache_spec),
        check_vma=False,
    )
```

```python
import functools

import jax
import jax.numpy as jnp
from jax import lax
from jax.experimental import pallas as pl
from jax.experimental.pallas import tpu as pltpu
from jax.sharding import PartitionSpec as P

F32 = jnp.float32
BF16 = jnp.bfloat16
MESH = pl.DeviceIdType.MESH
HBM = pl.BlockSpec(memory_space=pltpu.HBM)
VM = pl.BlockSpec(memory_space=pltpu.VMEM)
SM = pl.BlockSpec(memory_space=pltpu.SMEM)
DMA = pltpu.SemaphoreType.DMA


def dot(a, b):
    return jnp.dot(a, b, preferred_element_type=F32)


def place():
    m = lax.axis_index("model")
    return lax.axis_index("replica"), m, lax.rem(m, 2), m // 2


def greet(peers):
    barrier = pltpu.get_barrier_semaphore()
    for peer in peers:
        pl.semaphore_signal(barrier, inc=1, device_id=peer, device_id_type=MESH)


def meet(peers):
    pl.semaphore_wait(pltpu.get_barrier_semaphore(), len(peers))


def send(src, dst, send_sem, recv_sem, peer):
    return pltpu.make_async_remote_copy(
        src_ref=src, dst_ref=dst, send_sem=send_sem, recv_sem=recv_sem, device_id=peer, device_id_type=MESH)


def scatter_queries(get, qs, heads, rows):
    for h in range(heads):
        for i in range(2):
            qs[i, pl.ds(h, rows, stride=heads), :] = get(h)[:, i * 128:(i + 1) * 128].astype(F32)


def attend_rows(which, heads, length, kb, vb, qs, st, new=None, values=None):
    seq, dim = kb.shape[1:]
    scale = dim ** -0.5
    pos = lax.broadcasted_iota(jnp.int32, (heads, seq), 1)
    for b in which:
        cut = slice(b * heads, (b + 1) * heads)
        q = jnp.concatenate([qs[i, cut, :] for i in range(2)], axis=1)
        s = lax.dot_general(q.astype(BF16), kb[b], (((1,), (1,)), ((), ())), preferred_element_type=F32)
        if new is not None:
            s = jnp.where(pos == length(b), jnp.sum(q * new[0][b:b + 1, :], axis=1, keepdims=True), s)
        s = jnp.where(pos <= length(b), s * scale, -jnp.inf)
        for i in range(2):
            st[4 * i + b // 8, b % 8 * heads:(b % 8 + 1) * heads, :] = s[:, i * 256:(i + 1) * 256]
    if values is not None:
        values.wait()
    for b in which:
        cut = slice(b * heads, (b + 1) * heads)
        s = jnp.concatenate([st[4 * i + b // 8, b % 8 * heads:(b % 8 + 1) * heads, :] for i in range(2)], axis=1)
        e = jnp.exp(s - jnp.max(s, axis=1, keepdims=True))
        p = (e * (1.0 / jnp.sum(e, axis=1, keepdims=True))).astype(BF16)
        if new is None:
            c = dot(p, vb[b])
        else:
            here = pos == length(b)
            p = p.astype(F32)
            mine = jnp.sum(jnp.where(here, p, 0.0), axis=1, keepdims=True)
            c = dot(jnp.where(here, 0.0, p).astype(BF16), vb[b]) + mine * new[1][b:b + 1, :]
        for i in range(2):
            qs[i, cut, :] = c[:, i * 128:(i + 1) * 128]


def gather_contexts(ctx, qs, first, count, heads):
    for h in range(heads):
        for i in range(2):
            ctx[h, first:first + count, i * 128:(i + 1) * 128] = (
                qs[i, pl.ds(first * heads + h, count, stride=heads), :].astype(BF16))


def layer0_kernel(len_ref, x_hbm, wq_hbm, wk_hbm, wv_hbm, wo_hbm, kc_hbm, vc_hbm,
                  q_out, kvn, hl, wof, k0, v0, k1, v1,
                  xs, qown, qrecv, qs, ctx, wos, lhs, ys, yrecv, wq1, qacc, q1own, q1recv, stage,
                  wsem, lsem, c0sem, csem, qsem, gsem, psem, ysem, hsem, q1sem, xsem, yzsem, msem):
    rep, m, core, chip = place()
    heads, rows, dim = q_out.shape
    half = rows // 2
    chunks = hl.shape[0]
    across_m, mate_m, diag_m = 3 - m, m + 1 - 2 * core, lax.rem(m + 2, 4)
    across, mate, diag = (rep, across_m), (rep, mate_m), (rep, diag_m)
    rep_y, rep_z, rep_yz = rep + 1 - 2 * lax.rem(rep, 2), lax.rem(rep + 2, 4), 3 - rep
    next_y, next_z = (rep_y, m), (rep_z, m)
    span = wof.shape[2]
    quarter = stage.shape[0]
    subs = 4
    sub = quarter // subs

    def piece(owner, r, s):
        start = pl.multiple_of(lax.rem(r, 2) * quarter + s * sub, sub)
        return wof.at[2 * owner + r // 2, pl.ds(start, sub), :]

    friends = (across, diag, mate, next_y, next_z)
    greet(friends)
    xcopies = []

    def send_quarter(s):
        c = send(stage.at[pl.ds(s * sub, sub)], piece(m, rep, s), xsem.at[0, s], xsem.at[1, s], across)
        c.start()
        xcopies.append(c)

    around = []

    mcopies = []

    def to_mate(ref):
        n = len(mcopies)
        c = send(ref, ref, msem.at[0, n], msem.at[1, n], mate)
        c.start()
        mcopies.append(c)

    def pass_round(s):
        xcopies[s].wait_recv()
        ref = piece(across_m, rep, s)
        for n, peer in enumerate((next_y, next_z)):
            c = send(ref, ref, yzsem.at[0, n, s], yzsem.at[1, n, s], peer)
            c.start()
            around.append(c)

    load_x = pltpu.make_async_copy(x_hbm, xs, wsem.at[0])
    load_x.start()
    deep = k1.shape[1]
    blocks = xs.shape[1] // deep
    loads = []
    for n, src in enumerate((wq_hbm.at[0, :, pl.ds(0, dim)], wq_hbm.at[0, :, pl.ds(dim, dim)], wk_hbm.at[0], wv_hbm.at[0])):
        loads.append([pltpu.make_async_copy(src.at[pl.ds(t * deep, deep)], k1.at[n * blocks + t], lsem.at[n, t])
                      for t in range(blocks)])

    def start(copies):
        for c in copies:
            c.start()

    start(loads[0] + loads[1])

    def first_weights(n, rows_ref):
        total = None
        for c in loads[n]:
            c.wait()
        for t in range(blocks):
            part = dot(rows_ref[:, t * deep:(t + 1) * deep], k1[n * blocks + t])
            total = part if t == 0 else total + part
        return total.astype(BF16)

    theirs = pl.ds(pl.multiple_of((1 - chip) * span, span), span)
    ours = pl.ds(pl.multiple_of(chip * span, span), span)
    load_stage = pltpu.make_async_copy(
        wo_hbm.at[1, pl.ds(pl.multiple_of(rep * quarter, quarter), quarter), theirs], stage, wsem.at[5])
    load_stage.start()
    groups = [pl.ds(g * half, half) for g in range(2)]
    loads0 = [[pltpu.make_async_copy(src.at[0, groups[g]], dst.at[groups[g]], c0sem.at[g, n])
               for n, (src, dst) in enumerate(((kc_hbm, k0), (vc_hbm, v0)))] for g in range(2)]
    load_x.wait()
    start(loads[2] + loads[3])
    qcopies = []
    for i in range(2):
        q = first_weights(i, xs)
        if i == 0:
            start(loads0[0])
            meet(friends)
            load_stage.wait()
        for d in range(4):
            qown[d, i] = q[d * rows:(d + 1) * rows]
        for n, (peer, who) in enumerate(((across, across_m), (diag, diag_m), (mate, mate_m))):
            c = send(qown.at[who, i], qrecv.at[m, i], qsem.at[0, n, i], qsem.at[1, n, i], peer)
            c.start()
            qcopies.append(c)
        qrecv[m, i] = qown[m, i]
    load_wo = pltpu.make_async_copy(wo_hbm.at[0], wos.at[core], wsem.at[6])
    load_q1 = pltpu.make_async_copy(wq_hbm.at[1], wq1.at[core], wsem.at[7])
    load_own = [pltpu.make_async_copy(wo_hbm.at[1, pl.ds(i * dim, dim), ours], wof.at[2 * m + i], wsem.at[8 + i])
                for i in range(2)]
    start([load_wo] + loads0[1])
    for s in range(subs):
        send_quarter(s)
    mine = xs[pl.ds(pl.multiple_of(m * rows, rows), rows), :]
    kvn[0] = first_weights(2, mine).astype(F32)
    kvn[1] = first_weights(3, mine).astype(F32)
    for c in qcopies:
        c.wait()
    scatter_queries(lambda h: qrecv[h // 2, h % 2], qs, heads, rows)
    loads1 = [pltpu.make_async_copy(kc_hbm.at[1], k1, csem.at[0]), pltpu.make_async_copy(vc_hbm.at[1], v1, csem.at[1])]
    base = m * rows
    gives = []
    for g in range(2):
        loads0[g][0].wait()
        attend_rows(range(g * half, (g + 1) * half), heads, lambda b: len_ref[base + b], k0, v0, qs, ys,
                    (kvn.at[0], kvn.at[1]), loads0[g][1])
        gather_contexts(ctx, qs, g * half, half, heads)
        c = send(ctx.at[pl.ds((1 - chip) * 4, 4), pl.ds(g * half, half), :],
                 lhs.at[:, pl.ds(g * rows + half, half), :], gsem.at[0, g], gsem.at[1, g], across)
        c.start()
        gives.append(c)
        if g == 0:
            start([load_q1] + load_own)
            load_wo.wait()
            push_wo = send(wos.at[core], wos.at[core], psem.at[0, 0], psem.at[1, 0], mate)
            push_wo.start()
            pass_round(0)
    load_q1.wait()
    push_q1 = send(wq1.at[core], wq1.at[core], psem.at[0, 1], psem.at[1, 1], mate)
    push_q1.start()
    for i in range(2):
        load_own[i].wait()
        to_mate(wof.at[2 * m + i])
    start(loads1)
    to_mate(piece(across_m, rep, 0))
    for s in range(1, subs):
        pass_round(s)
        to_mate(piece(across_m, rep, s))
    for g in range(2):
        for i in range(4):
            lhs[i, g * rows:g * rows + half, :] = ctx[chip * 4 + i, g * half:(g + 1) * half, :]
    push_wo.wait()
    ycopies = []
    for g in range(2):
        gives[g].wait()
        both = slice(g * rows, (g + 1) * rows)
        for j in range(chunks):
            y = dot(lhs[0, both, :], wos[0, 0:256, j * 256:(j + 1) * 256])
            for i in range(1, 4):
                y += dot(lhs[i, both, :], wos[i // 2, (i % 2) * 256:(i % 2 + 1) * 256, j * 256:(j + 1) * 256])
            ys[j, both, :] = y
            n = g * chunks + j
            c = send(ys.at[j, pl.ds(g * rows + half, half)], yrecv.at[j, pl.ds(g * half, half)], ysem.at[0, n], ysem.at[1, n], across)
            c.start()
            ycopies.append(c)
    loads_kv = [[pltpu.make_async_copy(src.at[1, pl.ds(j * dim, dim)], wos.at[0, pl.ds(n * dim, dim), pl.ds(j * dim, dim)],
                                       lsem.at[4 + n, j]) for j in range(chunks)] for n, src in enumerate((wk_hbm, wv_hbm))]
    for c in loads_kv[0] + loads_kv[1]:
        c.start()
    for c in around:
        c.wait_recv()
    for s in range(subs):
        n, peer, other = ((1, next_z, rep_y), (0, next_y, rep_z))[s % 2]
        ref = piece(across_m, other, s)
        c = send(ref, ref, yzsem.at[0, n, subs + s // 2], yzsem.at[1, n, subs + s // 2], peer)
        c.start()
        around.append(c)
    for other in (rep_y, rep_z):
        for s in range(subs):
            to_mate(piece(across_m, other, s))
    hcopies = []
    for g in range(2):
        for j in range(chunks):
            n = g * chunks + j
            ycopies[n].wait_recv()
            part = slice(g * half, (g + 1) * half)
            old = xs[pl.ds(pl.multiple_of(m * rows + g * half, half), half), j * 256:(j + 1) * 256]
            hl[j, part, :] = (old.astype(F32) + (ys[j, g * rows:g * rows + half, :] + yrecv[j, part, :])).astype(BF16)
            c = send(hl.at[j, pl.ds(g * half, half)], hl.at[j, pl.ds(rows + g * half, half)], hsem.at[0, n], hsem.at[1, n], across)
            c.start()
            hcopies.append(c)
    push_q1.wait()
    for j in range(chunks):
        for g in range(2):
            hcopies[g * chunks + j].wait_recv()
        for i in range(4):
            part = dot(hl[j], wq1[i // 2, j * 256:(j + 1) * 256, (i % 2) * 256:(i % 2 + 1) * 256])
            if j == 0:
                qacc[i] = part
            else:
                qacc[i] += part
    q1copies = []
    for i in range(4):
        q1own[i] = qacc[i].astype(BF16)
        c = send(q1own.at[i, pl.ds(rows, rows)], q1recv.at[i], q1sem.at[0, i], q1sem.at[1, i], across)
        c.start()
        q1copies.append(c)
    for n in range(2):
        for j in range(chunks):
            loads_kv[n][j].wait()
            part = dot(hl[j, 0:rows, :], wos[0, n * dim:(n + 1) * dim, j * dim:(j + 1) * dim])
            t = part if j == 0 else t + part
        kvn[2 + n] = t.astype(BF16).astype(F32)
    for i in range(4):
        q_out[chip * 4 + i] = q1own[i, 0:rows, :]
    for s in range(subs):
        around[2 * subs + s].wait_recv()
    for s in range(subs):
        to_mate(piece(across_m, rep_yz, s))
    for i in range(4):
        q1copies[i].wait_recv()
        q_out[(1 - chip) * 4 + i] = q1recv[i]
    for c in mcopies:
        c.wait()
    for c in xcopies + around + ycopies + hcopies + q1copies:
        c.wait_send()
    for c in loads1:
        c.wait()


def write_out(bufs, ko, vo, layer, sems):
    outs = []
    for i in range(2):
        for n, (src, dst) in enumerate(zip(bufs, (ko, vo))):
            part = pl.ds(i * (src.shape[0] // 2), src.shape[0] // 2)
            c = pltpu.make_async_copy(src.at[part], dst.at[layer, part], sems.at[n, i])
            c.start()
            outs.append(c)
    return outs


def write1_kernel(k1, v1, _k, _v, ko, vo, osem):
    for c in write_out((k1, v1), ko, vo, 1, osem):
        c.wait()


def attend1_kernel(len_ref, q_ref, kvn, k0, v0, k1, v1, ctx, _k0, _v0, _k1, _v1, ko, vo, qs, st, osem):
    heads, rows, dim = q_ref.shape
    base = lax.axis_index("model") * rows
    tile = 16
    for layer, bufs in enumerate(((k0, v0), (k1, v1))):
        def patch(b, carry):
            ln = len_ref[base + b]
            start = pl.multiple_of((ln // tile) * tile, tile)
            hit = lax.broadcasted_iota(jnp.int32, (tile, dim), 0) == ln - start
            for n, buf in enumerate(bufs):
                old = buf[b, pl.ds(start, tile), :].astype(F32)
                buf[b, pl.ds(start, tile), :] = jnp.where(hit, kvn[2 * layer + n, pl.ds(b, 1), :], old).astype(BF16)
            return carry

        lax.fori_loop(0, rows, patch, 0, unroll=4)
        if layer == 0:
            outs = write_out(bufs, ko, vo, 0, osem)
    scatter_queries(lambda h: q_ref[h], qs, heads, rows)
    attend_rows(range(rows), heads, lambda b: len_ref[base + b], k1, v1, qs, st)
    gather_contexts(ctx, qs, 0, rows, heads)
    for c in outs:
        c.wait()


def last_kernel(ctx, other, hid, wof, out, left, hl, pl2, hsem, psem):
    rep, m, core, chip = place()
    across_m, mate_m, diag_m = 3 - m, m + 1 - 2 * core, lax.rem(m + 2, 4)
    across, mate = (rep, across_m), (rep, mate_m)
    heads, rows, dim = ctx.shape
    chunks = hl.shape[0]
    cols = chunks // 2
    greet((across, mate))
    hcopies = []
    pcopies = []

    def to_mate(at):
        n = len(pcopies)
        c = send(hl.at[at], pl2.at[at], psem.at[0, n], psem.at[1, n], mate)
        c.start()
        pcopies.append(c)

    for h in range(heads):
        left[h, 0:rows, :] = ctx[h]
        left[h, rows:2 * rows, :] = other[h]
    for j in range(cols):
        y = dot(left[0], wof[0, :, j * dim:(j + 1) * dim])
        for h in range(1, heads):
            y += dot(left[h], wof[h, :, j * dim:(j + 1) * dim])
        at = chip * cols + j
        hl[at] = (hid[at].astype(F32) + y).astype(BF16)
        if j == 0:
            meet((across, mate))
        for n in range(2):
            c = send(hl.at[at, pl.ds(n * rows, rows)], hl.at[at, pl.ds((1 - n) * rows, rows)],
                     hsem.at[0, n, j], hsem.at[1, n, j], across)
            c.start()
            hcopies.append(c)
        to_mate(at)
    for j in range(cols):
        for n in range(2):
            hcopies[2 * j + n].wait_recv()
        to_mate((1 - chip) * cols + j)

    def put(who, at, value):
        out[pl.ds(pl.multiple_of(who * rows, rows), rows), at * dim:(at + 1) * dim] = value

    for j in range(chunks):
        put(m, j, hl[j, 0:rows, :])
        put(across_m, j, hl[j, rows:2 * rows, :])
    for c in pcopies:
        c.wait_recv()
    for j in range(chunks):
        put(mate_m, j, pl2[j, 0:rows, :])
        put(diag_m, j, pl2[j, rows:2 * rows, :])
    for c in hcopies + pcopies:
        c.wait_send()


def solution(mesh):
    row_axes = ("replica", "model")
    cache_spec = P(None, row_axes, None, None)

    def device_step(x, cache_len, w_query, w_key, w_value, w_out, k_cache, v_cache):
        layers, rows, seq, dim = k_cache.shape
        total, width = x.shape
        chunks = width // dim
        local = w_query.shape[-1]
        heads = local // dim * mesh.shape["model"]
        hd = (heads, rows, dim)
        x, cache_len, w_query, w_key, w_value, w_out, k_cache, v_cache = (
            pltpu.with_memory_space_constraint(a, pltpu.HBM)
            for a in (x, cache_len, w_query, w_key, w_value, w_out, k_cache, v_cache))
        remote = functools.partial(pltpu.CompilerParams, has_side_effects=True)
        cache = pltpu.VMEM((rows, seq, dim), BF16)
        qs = pltpu.VMEM((2, rows * heads, 128), F32)
        st = pltpu.VMEM((chunks, 2 * rows, dim), F32)

        q, kvn, hid, wof, *caches = pl.pallas_call(
            layer0_kernel,
            out_shape=(pltpu.VMEM(hd, BF16), pltpu.VMEM((4, rows, dim), F32), pltpu.VMEM((chunks, 2 * rows, dim), BF16),
                       pltpu.VMEM((heads, dim, width // 2), BF16)) + (cache,) * 4,
            in_specs=[SM] + [HBM] * 7,
            out_specs=(VM,) * 8,
            scratch_shapes=[
                pltpu.VMEM((total, width), BF16),
                pltpu.VMEM((4, 2, rows, dim), BF16), pltpu.VMEM((4, 2, rows, dim), BF16),
                qs, pltpu.VMEM(hd, BF16),
                pltpu.VMEM((2, local, width), BF16), pltpu.VMEM((4, 2 * rows, dim), BF16),
                pltpu.VMEM((chunks, 2 * rows, dim), F32), pltpu.VMEM((chunks, rows, dim), F32),
                pltpu.VMEM((2, width, local), BF16),
                pltpu.VMEM((4, 2 * rows, dim), F32), pltpu.VMEM((4, 2 * rows, dim), BF16),
                pltpu.VMEM((4, rows, dim), BF16), pltpu.VMEM((local // 4, width // 2), BF16),
                DMA((10,)), DMA((6, 8)), DMA((2, 2)), DMA((2,)), DMA((2, 3, 2)), DMA((2, 2)), DMA((2, 2)), DMA((2, 2 * chunks)), DMA((2, 2 * chunks)),
                DMA((2, 4)), DMA((2, 4)), DMA((2, 2, 6)), DMA((2, 18)),
            ],
            compiler_params=remote(collective_id=0, vmem_limit_bytes=11 << 20),
            name="layer0",
        )(cache_len, x, w_query, w_key, w_value, w_out, k_cache, v_cache)

        ctx, _, _, k1, v1, ko, vo = pl.pallas_call(
            attend1_kernel,
            out_shape=(pltpu.VMEM(hd, BF16), cache, cache, cache, cache,
                       jax.ShapeDtypeStruct(k_cache.shape, BF16), jax.ShapeDtypeStruct(v_cache.shape, BF16)),
            in_specs=[SM] + [VM] * 6,
            out_specs=(VM,) * 5 + (HBM, HBM),
            input_output_aliases={3: 1, 4: 2, 5: 3, 6: 4},
            scratch_shapes=[qs, st, DMA((2, 2))],
            compiler_params=pltpu.CompilerParams(vmem_limit_bytes=3 << 20),
            name="attend1",
        )(cache_len, q, kvn, *caches)

        other = lax.ppermute(ctx, "model", [(i, 3 - i) for i in range(4)])
        ko, vo = pl.pallas_call(
            write1_kernel,
            out_shape=(jax.ShapeDtypeStruct(k_cache.shape, BF16), jax.ShapeDtypeStruct(v_cache.shape, BF16)),
            in_specs=[VM, VM, HBM, HBM],
            out_specs=(HBM, HBM),
            input_output_aliases={2: 0, 3: 1},
            scratch_shapes=[DMA((2, 2))],
            compiler_params=pltpu.CompilerParams(vmem_limit_bytes=1 << 20),
            cost_estimate=pl.CostEstimate(flops=10 ** 9, bytes_accessed=2 ** 25, transcendentals=0),
            name="write1",
        )(k1, v1, ko, vo)

        out = pl.pallas_call(
            last_kernel,
            out_shape=pltpu.VMEM((total, width), BF16),
            in_specs=[VM] * 4,
            out_specs=VM,
            scratch_shapes=[
                pltpu.VMEM((heads, 2 * rows, dim), BF16),
                pltpu.VMEM((chunks, 2 * rows, dim), BF16), pltpu.VMEM((chunks, 2 * rows, dim), BF16),
                DMA((2, 2, chunks // 2)), DMA((2, chunks)),
            ],
            compiler_params=remote(collective_id=1, vmem_limit_bytes=4 << 20),
            name="last",
        )(ctx, other, hid, wof)
        return out, ko, vo

    return jax.shard_map(
        device_step,
        mesh=mesh,
        in_specs=(P("replica", None), P("replica"), P(None, None, "model"), P(), P(), P(None, "model", None), cache_spec, cache_spec),
        out_specs=(P("replica", None), cache_spec, cache_spec),
        check_vma=False,
    )
```

```python
import functools

import jax
import jax.numpy as jnp
from jax import lax
from jax.experimental import pallas as pl
from jax.experimental.pallas import tpu as pltpu
from jax.sharding import PartitionSpec as P

F32 = jnp.float32
BF16 = jnp.bfloat16
MESH = pl.DeviceIdType.MESH
HBM = pl.BlockSpec(memory_space=pltpu.HBM)
VM = pl.BlockSpec(memory_space=pltpu.VMEM)
SM = pl.BlockSpec(memory_space=pltpu.SMEM)
DMA = pltpu.SemaphoreType.DMA


def dot(a, b):
    return jnp.dot(a, b, preferred_element_type=F32)


def place():
    m = lax.axis_index("model")
    return lax.axis_index("replica"), m, lax.rem(m, 2), m // 2


def greet(peers):
    barrier = pltpu.get_barrier_semaphore()
    for peer in peers:
        pl.semaphore_signal(barrier, inc=1, device_id=peer, device_id_type=MESH)


def meet(peers):
    pl.semaphore_wait(pltpu.get_barrier_semaphore(), len(peers))


def send(src, dst, send_sem, recv_sem, peer):
    return pltpu.make_async_remote_copy(
        src_ref=src, dst_ref=dst, send_sem=send_sem, recv_sem=recv_sem, device_id=peer, device_id_type=MESH)


LAG = 8


def scatter_queries(get, qs, heads, rows):
    for h in range(heads):
        for i in range(2):
            qs[i, pl.ds(h, rows, stride=heads), :] = get(h)[:, i * 128:(i + 1) * 128].astype(F32)


def attend_rows(which, heads, length, kb, vb, qs, new=None):
    seq, dim = kb.shape[1:]
    scale = dim ** -0.5
    pos = lax.broadcasted_iota(jnp.int32, (heads, seq), 1)
    waiting = []
    for b in list(which) + [None] * LAG:
        if b is not None:
            cut = slice(b * heads, (b + 1) * heads)
            q = jnp.concatenate([qs[i, cut, :] for i in range(2)], axis=1)
            s = lax.dot_general(q.astype(BF16), kb[b], (((1,), (1,)), ((), ())), preferred_element_type=F32)
            if new is not None:
                s = jnp.where(pos == length(b), jnp.sum(q * new[0][b:b + 1, :], axis=1, keepdims=True), s)
            waiting.append((b, jnp.where(pos <= length(b), s * scale, -jnp.inf)))
        if b is not None and len(waiting) <= LAG:
            continue
        if not waiting:
            continue
        b, s = waiting.pop(0)
        cut = slice(b * heads, (b + 1) * heads)
        e = jnp.exp(s - jnp.max(s, axis=1, keepdims=True))
        p = (e * (1.0 / jnp.sum(e, axis=1, keepdims=True))).astype(BF16)
        if new is None:
            c = dot(p, vb[b])
        else:
            here = pos == length(b)
            p = p.astype(F32)
            mine = jnp.sum(jnp.where(here, p, 0.0), axis=1, keepdims=True)
            c = dot(jnp.where(here, 0.0, p).astype(BF16), vb[b]) + mine * new[1][b:b + 1, :]
        for i in range(2):
            qs[i, cut, :] = c[:, i * 128:(i + 1) * 128]


def gather_contexts(ctx, qs, first, count, heads):
    for h in range(heads):
        for i in range(2):
            ctx[h, first:first + count, i * 128:(i + 1) * 128] = (
                qs[i, pl.ds(first * heads + h, count, stride=heads), :].astype(BF16))


def layer0_kernel(len_ref, x_hbm, wq_hbm, wk_hbm, wv_hbm, wo_hbm, kc_hbm, vc_hbm,
                  q_out, kvn, hl, wof, k0, v0, k1, v1,
                  xs, qown, qrecv, qs, ctx, wos, lhs, ys, yrecv, wq1, qacc, q1own, q1recv, stage,
                  wsem, lsem, c0sem, csem, qsem, gsem, psem, ysem, hsem, q1sem, xsem, yzsem, msem):
    rep, m, core, chip = place()
    heads, rows, dim = q_out.shape
    half = rows // 2
    chunks = hl.shape[0]
    across_m, mate_m, diag_m = 3 - m, m + 1 - 2 * core, lax.rem(m + 2, 4)
    across, mate, diag = (rep, across_m), (rep, mate_m), (rep, diag_m)
    rep_y, rep_z, rep_yz = rep + 1 - 2 * lax.rem(rep, 2), lax.rem(rep + 2, 4), 3 - rep
    next_y, next_z = (rep_y, m), (rep_z, m)
    span = wof.shape[2]
    quarter = stage.shape[0]
    subs = 4
    sub = quarter // subs

    def piece(owner, r, s):
        start = pl.multiple_of(lax.rem(r, 2) * quarter + s * sub, sub)
        return wof.at[2 * owner + r // 2, pl.ds(start, sub), :]

    friends = (across, diag, mate, next_y, next_z)
    greet(friends)
    xcopies = []

    def send_quarter(s):
        c = send(stage.at[pl.ds(s * sub, sub)], piece(m, rep, s), xsem.at[0, s], xsem.at[1, s], across)
        c.start()
        xcopies.append(c)

    around = []

    mcopies = []

    def to_mate(ref):
        n = len(mcopies)
        c = send(ref, ref, msem.at[0, n], msem.at[1, n], mate)
        c.start()
        mcopies.append(c)

    def pass_round(s):
        xcopies[s].wait_recv()
        ref = piece(across_m, rep, s)
        for n, peer in enumerate((next_y, next_z)):
            c = send(ref, ref, yzsem.at[0, n, s], yzsem.at[1, n, s], peer)
            c.start()
            around.append(c)

    load_x = pltpu.make_async_copy(x_hbm, xs, wsem.at[0])
    load_x.start()
    deep = k1.shape[1]
    blocks = xs.shape[1] // deep
    loads = []
    for n, src in enumerate((wq_hbm.at[0, :, pl.ds(0, dim)], wq_hbm.at[0, :, pl.ds(dim, dim)], wk_hbm.at[0], wv_hbm.at[0])):
        loads.append([pltpu.make_async_copy(src.at[pl.ds(t * deep, deep)], k1.at[n * blocks + t], lsem.at[n, t])
                      for t in range(blocks)])

    def start(copies):
        for c in copies:
            c.start()

    start(loads[0] + loads[1])

    def first_weights(n, rows_ref):
        total = None
        for c in loads[n]:
            c.wait()
        for t in range(blocks):
            part = dot(rows_ref[:, t * deep:(t + 1) * deep], k1[n * blocks + t])
            total = part if t == 0 else total + part
        return total.astype(BF16)

    theirs = pl.ds(pl.multiple_of((1 - chip) * span, span), span)
    ours = pl.ds(pl.multiple_of(chip * span, span), span)
    load_stage = pltpu.make_async_copy(
        wo_hbm.at[1, pl.ds(pl.multiple_of(rep * quarter, quarter), quarter), theirs], stage, wsem.at[5])
    load_stage.start()
    groups = [pl.ds(g * half, half) for g in range(2)]
    loads0 = [[pltpu.make_async_copy(src.at[0, groups[g]], dst.at[groups[g]], c0sem.at[g, n])
               for n, (src, dst) in enumerate(((kc_hbm, k0), (vc_hbm, v0)))] for g in range(2)]
    load_wo = pltpu.make_async_copy(wo_hbm.at[0], wos.at[core], wsem.at[6])
    load_x.wait()
    start(loads[2] + loads[3] + loads0[0])
    qcopies = []
    for i in range(2):
        q = first_weights(i, xs)
        if i == 0:
            start([load_wo] + loads0[1])
            meet(friends)
            load_stage.wait()
        for d in range(4):
            qown[d, i] = q[d * rows:(d + 1) * rows]
        for n, (peer, who) in enumerate(((across, across_m), (diag, diag_m), (mate, mate_m))):
            c = send(qown.at[who, i], qrecv.at[m, i], qsem.at[0, n, i], qsem.at[1, n, i], peer)
            c.start()
            qcopies.append(c)
        qrecv[m, i] = qown[m, i]
    load_q1 = pltpu.make_async_copy(wq_hbm.at[1], wq1.at[core], wsem.at[7])
    load_own = [pltpu.make_async_copy(wo_hbm.at[1, pl.ds(i * dim, dim), ours], wof.at[2 * m + i], wsem.at[8 + i])
                for i in range(2)]
    for s in range(subs):
        send_quarter(s)
    mine = xs[pl.ds(pl.multiple_of(m * rows, rows), rows), :]
    kvn[0] = first_weights(2, mine).astype(F32)
    kvn[1] = first_weights(3, mine).astype(F32)
    for c in qcopies:
        c.wait()
    scatter_queries(lambda h: qrecv[h // 2, h % 2], qs, heads, rows)
    loads1 = [pltpu.make_async_copy(kc_hbm.at[1], k1, csem.at[0]), pltpu.make_async_copy(vc_hbm.at[1], v1, csem.at[1])]
    base = m * rows
    gives = []
    for g in range(2):
        for c in loads0[g]:
            c.wait()
        attend_rows(range(g * half, (g + 1) * half), heads, lambda b: len_ref[base + b], k0, v0, qs, (kvn.at[0], kvn.at[1]))
        gather_contexts(ctx, qs, g * half, half, heads)
        c = send(ctx.at[pl.ds((1 - chip) * 4, 4), pl.ds(g * half, half), :],
                 lhs.at[:, pl.ds(g * rows + half, half), :], gsem.at[0, g], gsem.at[1, g], across)
        c.start()
        gives.append(c)
        if g == 0:
            start([load_q1] + load_own)
            load_wo.wait()
            push_wo = send(wos.at[core], wos.at[core], psem.at[0, 0], psem.at[1, 0], mate)
            push_wo.start()
            pass_round(0)
    load_q1.wait()
    push_q1 = send(wq1.at[core], wq1.at[core], psem.at[0, 1], psem.at[1, 1], mate)
    push_q1.start()
    for i in range(2):
        load_own[i].wait()
        to_mate(wof.at[2 * m + i])
    start(loads1)
    to_mate(piece(across_m, rep, 0))
    for s in range(1, subs):
        pass_round(s)
        to_mate(piece(across_m, rep, s))
    for g in range(2):
        for i in range(4):
            lhs[i, g * rows:g * rows + half, :] = ctx[chip * 4 + i, g * half:(g + 1) * half, :]
    push_wo.wait()
    ycopies = []
    for g in range(2):
        gives[g].wait()
        both = slice(g * rows, (g + 1) * rows)
        for j in range(chunks):
            y = dot(lhs[0, both, :], wos[0, 0:256, j * 256:(j + 1) * 256])
            for i in range(1, 4):
                y += dot(lhs[i, both, :], wos[i // 2, (i % 2) * 256:(i % 2 + 1) * 256, j * 256:(j + 1) * 256])
            ys[j, both, :] = y
            n = g * chunks + j
            c = send(ys.at[j, pl.ds(g * rows + half, half)], yrecv.at[j, pl.ds(g * half, half)], ysem.at[0, n], ysem.at[1, n], across)
            c.start()
            ycopies.append(c)
    loads_kv = [[pltpu.make_async_copy(src.at[1, pl.ds(j * dim, dim)], wos.at[0, pl.ds(n * dim, dim), pl.ds(j * dim, dim)],
                                       lsem.at[4 + n, j]) for j in range(chunks)] for n, src in enumerate((wk_hbm, wv_hbm))]
    for c in loads_kv[0] + loads_kv[1]:
        c.start()
    for c in around:
        c.wait_recv()
    for s in range(subs):
        n, peer, other = ((1, next_z, rep_y), (0, next_y, rep_z))[s % 2]
        ref = piece(across_m, other, s)
        c = send(ref, ref, yzsem.at[0, n, subs + s // 2], yzsem.at[1, n, subs + s // 2], peer)
        c.start()
        around.append(c)
    for other in (rep_y, rep_z):
        for s in range(subs):
            to_mate(piece(across_m, other, s))
    hcopies = []
    for g in range(2):
        for j in range(chunks):
            n = g * chunks + j
            ycopies[n].wait_recv()
            part = slice(g * half, (g + 1) * half)
            old = xs[pl.ds(pl.multiple_of(m * rows + g * half, half), half), j * 256:(j + 1) * 256]
            hl[j, part, :] = (old.astype(F32) + (ys[j, g * rows:g * rows + half, :] + yrecv[j, part, :])).astype(BF16)
            c = send(hl.at[j, pl.ds(g * half, half)], hl.at[j, pl.ds(rows + g * half, half)], hsem.at[0, n], hsem.at[1, n], across)
            c.start()
            hcopies.append(c)
    push_q1.wait()
    for j in range(chunks):
        for g in range(2):
            hcopies[g * chunks + j].wait_recv()
        for i in range(4):
            part = dot(hl[j], wq1[i // 2, j * 256:(j + 1) * 256, (i % 2) * 256:(i % 2 + 1) * 256])
            if j == 0:
                qacc[i] = part
            else:
                qacc[i] += part
    q1copies = []
    for i in range(4):
        q1own[i] = qacc[i].astype(BF16)
        c = send(q1own.at[i, pl.ds(rows, rows)], q1recv.at[i], q1sem.at[0, i], q1sem.at[1, i], across)
        c.start()
        q1copies.append(c)
    for n in range(2):
        for j in range(chunks):
            loads_kv[n][j].wait()
            part = dot(hl[j, 0:rows, :], wos[0, n * dim:(n + 1) * dim, j * dim:(j + 1) * dim])
            t = part if j == 0 else t + part
        kvn[2 + n] = t.astype(BF16).astype(F32)
    for i in range(4):
        q_out[chip * 4 + i] = q1own[i, 0:rows, :]
    for s in range(subs):
        around[2 * subs + s].wait_recv()
    for s in range(subs):
        to_mate(piece(across_m, rep_yz, s))
    for i in range(4):
        q1copies[i].wait_recv()
        q_out[(1 - chip) * 4 + i] = q1recv[i]
    for c in mcopies:
        c.wait()
    for c in xcopies + around + ycopies + hcopies + q1copies:
        c.wait_send()
    for c in loads1:
        c.wait()


PARTS = 4


def write_out(buf, out, layer, sems):
    copies = []
    count = buf.shape[0] // PARTS
    for i in range(PARTS):
        part = pl.ds(i * count, count)
        c = pltpu.make_async_copy(buf.at[part], out.at[layer, part], sems.at[i])
        c.start()
        copies.append(c)
    return copies


def write1_kernel(k1, v1, _k, _v, ko, vo, osem):
    for c in write_out(k1, ko, 1, osem.at[0]) + write_out(v1, vo, 1, osem.at[1]):
        c.wait()


def attend1_kernel(len_ref, q_ref, kvn, k0, v0, k1, v1, ctx, _k0, _v0, _k1, _v1, ko, vo, qs, osem):
    heads, rows, dim = q_ref.shape
    base = lax.axis_index("model") * rows
    tile = 16
    outs = []
    for n, buf in enumerate((k0, v0, k1, v1)):
        def patch(b, carry):
            ln = len_ref[base + b]
            start = pl.multiple_of((ln // tile) * tile, tile)
            hit = lax.broadcasted_iota(jnp.int32, (tile, dim), 0) == ln - start
            old = buf[b, pl.ds(start, tile), :].astype(F32)
            buf[b, pl.ds(start, tile), :] = jnp.where(hit, kvn[n, pl.ds(b, 1), :], old).astype(BF16)
            return carry

        lax.fori_loop(0, rows, patch, 0, unroll=8)
        if n < 2:
            outs += write_out(buf, (ko, vo)[n], 0, osem.at[n])
    scatter_queries(lambda h: q_ref[h], qs, heads, rows)
    attend_rows(range(rows), heads, lambda b: len_ref[base + b], k1, v1, qs)
    gather_contexts(ctx, qs, 0, rows, heads)
    for c in outs:
        c.wait()


def last_kernel(ctx, other, hid, wof, out, left, hl, pl2, hsem, psem):
    rep, m, core, chip = place()
    across_m, mate_m, diag_m = 3 - m, m + 1 - 2 * core, lax.rem(m + 2, 4)
    across, mate = (rep, across_m), (rep, mate_m)
    heads, rows, dim = ctx.shape
    chunks = hl.shape[0]
    cols = chunks // 2
    greet((across, mate))
    hcopies = []
    pcopies = []

    def to_mate(at):
        n = len(pcopies)
        c = send(hl.at[at], pl2.at[at], psem.at[0, n], psem.at[1, n], mate)
        c.start()
        pcopies.append(c)

    for h in range(heads):
        left[h, 0:rows, :] = ctx[h]
        left[h, rows:2 * rows, :] = other[h]
    for j in range(cols):
        y = dot(left[0], wof[0, :, j * dim:(j + 1) * dim])
        for h in range(1, heads):
            y += dot(left[h], wof[h, :, j * dim:(j + 1) * dim])
        at = chip * cols + j
        hl[at] = (hid[at].astype(F32) + y).astype(BF16)
        if j == 0:
            meet((across, mate))
        for n in range(2):
            c = send(hl.at[at, pl.ds(n * rows, rows)], hl.at[at, pl.ds((1 - n) * rows, rows)],
                     hsem.at[0, n, j], hsem.at[1, n, j], across)
            c.start()
            hcopies.append(c)
        to_mate(at)
    for j in range(cols):
        for n in range(2):
            hcopies[2 * j + n].wait_recv()
        to_mate((1 - chip) * cols + j)

    def put(who, at, value):
        out[pl.ds(pl.multiple_of(who * rows, rows), rows), at * dim:(at + 1) * dim] = value

    for j in range(chunks):
        put(m, j, hl[j, 0:rows, :])
        put(across_m, j, hl[j, rows:2 * rows, :])
    for c in pcopies:
        c.wait_recv()
    for j in range(chunks):
        put(mate_m, j, pl2[j, 0:rows, :])
        put(diag_m, j, pl2[j, rows:2 * rows, :])
    for c in hcopies + pcopies:
        c.wait_send()


def solution(mesh):
    row_axes = ("replica", "model")
    cache_spec = P(None, row_axes, None, None)

    def device_step(x, cache_len, w_query, w_key, w_value, w_out, k_cache, v_cache):
        layers, rows, seq, dim = k_cache.shape
        total, width = x.shape
        chunks = width // dim
        local = w_query.shape[-1]
        heads = local // dim * mesh.shape["model"]
        hd = (heads, rows, dim)
        x, cache_len, w_query, w_key, w_value, w_out, k_cache, v_cache = (
            pltpu.with_memory_space_constraint(a, pltpu.HBM)
            for a in (x, cache_len, w_query, w_key, w_value, w_out, k_cache, v_cache))
        remote = functools.partial(pltpu.CompilerParams, has_side_effects=True)
        cache = pltpu.VMEM((rows, seq, dim), BF16)
        qs = pltpu.VMEM((2, rows * heads, 128), F32)

        q, kvn, hid, wof, *caches = pl.pallas_call(
            layer0_kernel,
            out_shape=(pltpu.VMEM(hd, BF16), pltpu.VMEM((4, rows, dim), F32), pltpu.VMEM((chunks, 2 * rows, dim), BF16),
                       pltpu.VMEM((heads, dim, width // 2), BF16)) + (cache,) * 4,
            in_specs=[SM] + [HBM] * 7,
            out_specs=(VM,) * 8,
            scratch_shapes=[
                pltpu.VMEM((total, width), BF16),
                pltpu.VMEM((4, 2, rows, dim), BF16), pltpu.VMEM((4, 2, rows, dim), BF16),
                qs, pltpu.VMEM(hd, BF16),
                pltpu.VMEM((2, local, width), BF16), pltpu.VMEM((4, 2 * rows, dim), BF16),
                pltpu.VMEM((chunks, 2 * rows, dim), F32), pltpu.VMEM((chunks, rows, dim), F32),
                pltpu.VMEM((2, width, local), BF16),
                pltpu.VMEM((4, 2 * rows, dim), F32), pltpu.VMEM((4, 2 * rows, dim), BF16),
                pltpu.VMEM((4, rows, dim), BF16), pltpu.VMEM((local // 4, width // 2), BF16),
                DMA((10,)), DMA((6, 8)), DMA((2, 2)), DMA((2,)), DMA((2, 3, 2)), DMA((2, 2)), DMA((2, 2)), DMA((2, 2 * chunks)), DMA((2, 2 * chunks)),
                DMA((2, 4)), DMA((2, 4)), DMA((2, 2, 6)), DMA((2, 18)),
            ],
            compiler_params=remote(collective_id=0, vmem_limit_bytes=11 << 20),
            name="layer0",
        )(cache_len, x, w_query, w_key, w_value, w_out, k_cache, v_cache)

        ctx, _, _, k1, v1, ko, vo = pl.pallas_call(
            attend1_kernel,
            out_shape=(pltpu.VMEM(hd, BF16), cache, cache, cache, cache,
                       jax.ShapeDtypeStruct(k_cache.shape, BF16), jax.ShapeDtypeStruct(v_cache.shape, BF16)),
            in_specs=[SM] + [VM] * 6,
            out_specs=(VM,) * 5 + (HBM, HBM),
            input_output_aliases={3: 1, 4: 2, 5: 3, 6: 4},
            scratch_shapes=[qs, DMA((2, PARTS))],
            compiler_params=pltpu.CompilerParams(vmem_limit_bytes=3 << 20),
            name="attend1",
        )(cache_len, q, kvn, *caches)

        other = lax.ppermute(ctx, "model", [(i, 3 - i) for i in range(4)])
        ko, vo = pl.pallas_call(
            write1_kernel,
            out_shape=(jax.ShapeDtypeStruct(k_cache.shape, BF16), jax.ShapeDtypeStruct(v_cache.shape, BF16)),
            in_specs=[VM, VM, HBM, HBM],
            out_specs=(HBM, HBM),
            input_output_aliases={2: 0, 3: 1},
            scratch_shapes=[DMA((2, PARTS))],
            compiler_params=pltpu.CompilerParams(vmem_limit_bytes=1 << 20),
            cost_estimate=pl.CostEstimate(flops=10 ** 9, bytes_accessed=2 ** 25, transcendentals=0),
            name="write1",
        )(k1, v1, ko, vo)

        out = pl.pallas_call(
            last_kernel,
            out_shape=pltpu.VMEM((total, width), BF16),
            in_specs=[VM] * 4,
            out_specs=VM,
            scratch_shapes=[
                pltpu.VMEM((heads, 2 * rows, dim), BF16),
                pltpu.VMEM((chunks, 2 * rows, dim), BF16), pltpu.VMEM((chunks, 2 * rows, dim), BF16),
                DMA((2, 2, chunks // 2)), DMA((2, chunks)),
            ],
            compiler_params=remote(collective_id=1, vmem_limit_bytes=4 << 20),
            name="last",
        )(ctx, other, hid, wof)
        return out, ko, vo

    return jax.shard_map(
        device_step,
        mesh=mesh,
        in_specs=(P("replica", None), P("replica"), P(None, None, "model"), P(), P(), P(None, "model", None), cache_spec, cache_spec),
        out_specs=(P("replica", None), cache_spec, cache_spec),
        check_vma=False,
    )
```

```python
import functools

import jax
import jax.numpy as jnp
from jax import lax
from jax.experimental import pallas as pl
from jax.experimental.pallas import tpu as pltpu
from jax.sharding import PartitionSpec as P

F32 = jnp.float32
BF16 = jnp.bfloat16
MESH = pl.DeviceIdType.MESH
HBM = pl.BlockSpec(memory_space=pltpu.HBM)
VM = pl.BlockSpec(memory_space=pltpu.VMEM)
SM = pl.BlockSpec(memory_space=pltpu.SMEM)
DMA = pltpu.SemaphoreType.DMA


def dot(a, b):
    return jnp.dot(a, b, preferred_element_type=F32)


def place():
    m = lax.axis_index("model")
    return lax.axis_index("replica"), m, lax.rem(m, 2), m // 2


def greet(peers):
    barrier = pltpu.get_barrier_semaphore()
    for peer in peers:
        pl.semaphore_signal(barrier, inc=1, device_id=peer, device_id_type=MESH)


def meet(peers):
    pl.semaphore_wait(pltpu.get_barrier_semaphore(), len(peers))


def send(src, dst, send_sem, recv_sem, peer):
    return pltpu.make_async_remote_copy(
        src_ref=src, dst_ref=dst, send_sem=send_sem, recv_sem=recv_sem, device_id=peer, device_id_type=MESH)


LAG = 12
YSTEP = 1
HSTEP = 2


def scatter_queries(get, qs, heads, rows):
    for h in range(heads):
        for i in range(2):
            qs[i, pl.ds(h, rows, stride=heads), :] = get(h)[:, i * 128:(i + 1) * 128].astype(F32)


def attend_rows(which, heads, length, kb, vb, qs, new=None):
    seq, dim = kb.shape[1:]
    scale = dim ** -0.5
    pos = lax.broadcasted_iota(jnp.int32, (heads, seq), 1)
    waiting = []
    for b in list(which) + [None] * LAG:
        if b is not None:
            cut = slice(b * heads, (b + 1) * heads)
            q = jnp.concatenate([qs[i, cut, :] for i in range(2)], axis=1)
            s = lax.dot_general(q.astype(BF16), kb[b], (((1,), (1,)), ((), ())), preferred_element_type=F32)
            if new is not None:
                s = jnp.where(pos == length(b), jnp.sum(q * new[0][b:b + 1, :], axis=1, keepdims=True), s)
            waiting.append((b, jnp.where(pos <= length(b), s * scale, -jnp.inf)))
        if b is not None and len(waiting) <= LAG:
            continue
        if not waiting:
            continue
        b, s = waiting.pop(0)
        cut = slice(b * heads, (b + 1) * heads)
        e = jnp.exp(s - jnp.max(s, axis=1, keepdims=True))
        p = (e * (1.0 / jnp.sum(e, axis=1, keepdims=True))).astype(BF16)
        if new is None:
            c = dot(p, vb[b])
        else:
            here = pos == length(b)
            p = p.astype(F32)
            mine = jnp.sum(jnp.where(here, p, 0.0), axis=1, keepdims=True)
            c = dot(jnp.where(here, 0.0, p).astype(BF16), vb[b]) + mine * new[1][b:b + 1, :]
        for i in range(2):
            qs[i, cut, :] = c[:, i * 128:(i + 1) * 128]


def gather_contexts(ctx, qs, first, count, heads):
    for h in range(heads):
        for i in range(2):
            ctx[h, first:first + count, i * 128:(i + 1) * 128] = (
                qs[i, pl.ds(first * heads + h, count, stride=heads), :].astype(BF16))


def layer0_kernel(len_ref, x_hbm, wq_hbm, wk_hbm, wv_hbm, wo_hbm, kc_hbm, vc_hbm,
                  q_out, kvn, hl, wof, k0, v0, k1, v1,
                  xs, qown, qrecv, qs, ctx, wos, lhs, ys, yrecv, wq1, qacc, q1own, q1recv, stage,
                  wsem, lsem, c0sem, csem, qsem, gsem, psem, ysem, hsem, q1sem, xsem, yzsem, msem):
    rep, m, core, chip = place()
    heads, rows, dim = q_out.shape
    half = rows // 2
    chunks = hl.shape[0]
    across_m, mate_m, diag_m = 3 - m, m + 1 - 2 * core, lax.rem(m + 2, 4)
    across, mate, diag = (rep, across_m), (rep, mate_m), (rep, diag_m)
    rep_y, rep_z, rep_yz = rep + 1 - 2 * lax.rem(rep, 2), lax.rem(rep + 2, 4), 3 - rep
    next_y, next_z = (rep_y, m), (rep_z, m)
    span = wof.shape[2]
    quarter = stage.shape[0]
    subs = 4
    sub = quarter // subs

    def piece(owner, r, s):
        start = pl.multiple_of(lax.rem(r, 2) * quarter + s * sub, sub)
        return wof.at[2 * owner + r // 2, pl.ds(start, sub), :]

    friends = (across, diag, mate, next_y, next_z)
    greet(friends)
    xcopies = []

    def send_quarter(s):
        c = send(stage.at[pl.ds(s * sub, sub)], piece(m, rep, s), xsem.at[0, s], xsem.at[1, s], across)
        c.start()
        xcopies.append(c)

    around = []

    mcopies = []

    def to_mate(ref):
        n = len(mcopies)
        c = send(ref, ref, msem.at[0, n], msem.at[1, n], mate)
        c.start()
        mcopies.append(c)

    def pass_round(s):
        xcopies[s].wait_recv()
        ref = piece(across_m, rep, s)
        for n, peer in enumerate((next_y, next_z)):
            c = send(ref, ref, yzsem.at[0, n, s], yzsem.at[1, n, s], peer)
            c.start()
            around.append(c)

    load_x = pltpu.make_async_copy(x_hbm, xs, wsem.at[0])
    load_x.start()
    deep = k1.shape[1]
    blocks = xs.shape[1] // deep
    loads = []
    for n, src in enumerate((wq_hbm.at[0, :, pl.ds(0, dim)], wq_hbm.at[0, :, pl.ds(dim, dim)], wk_hbm.at[0], wv_hbm.at[0])):
        loads.append([pltpu.make_async_copy(src.at[pl.ds(t * deep, deep)], k1.at[n * blocks + t], lsem.at[n, t])
                      for t in range(blocks)])

    def start(copies):
        for c in copies:
            c.start()

    start(loads[0] + loads[1])

    def first_weights(n, rows_ref):
        total = None
        for c in loads[n]:
            c.wait()
        for t in range(blocks):
            part = dot(rows_ref[:, t * deep:(t + 1) * deep], k1[n * blocks + t])
            total = part if t == 0 else total + part
        return total.astype(BF16)

    theirs = pl.ds(pl.multiple_of((1 - chip) * span, span), span)
    ours = pl.ds(pl.multiple_of(chip * span, span), span)
    load_stage = pltpu.make_async_copy(
        wo_hbm.at[1, pl.ds(pl.multiple_of(rep * quarter, quarter), quarter), theirs], stage, wsem.at[5])
    load_stage.start()
    groups = [pl.ds(g * half, half) for g in range(2)]
    loads0 = [[pltpu.make_async_copy(src.at[0, groups[g]], dst.at[groups[g]], c0sem.at[g, n])
               for n, (src, dst) in enumerate(((kc_hbm, k0), (vc_hbm, v0)))] for g in range(2)]
    load_wo = pltpu.make_async_copy(wo_hbm.at[0], wos.at[core], wsem.at[6])
    load_x.wait()
    start(loads[2] + loads[3] + loads0[0])
    qcopies = []
    for i in range(2):
        q = first_weights(i, xs)
        if i == 0:
            start([load_wo] + loads0[1])
            meet(friends)
            load_stage.wait()
        for d in range(4):
            qown[d, i] = q[d * rows:(d + 1) * rows]
        for n, (peer, who) in enumerate(((across, across_m), (diag, diag_m), (mate, mate_m))):
            c = send(qown.at[who, i], qrecv.at[m, i], qsem.at[0, n, i], qsem.at[1, n, i], peer)
            c.start()
            qcopies.append(c)
        qrecv[m, i] = qown[m, i]
    load_q1 = pltpu.make_async_copy(wq_hbm.at[1], wq1.at[core], wsem.at[7])
    load_own = [pltpu.make_async_copy(wo_hbm.at[1, pl.ds(i * dim, dim), ours], wof.at[2 * m + i], wsem.at[8 + i])
                for i in range(2)]
    for s in range(subs):
        send_quarter(s)
    mine = xs[pl.ds(pl.multiple_of(m * rows, rows), rows), :]
    kvn[0] = first_weights(2, mine).astype(F32)
    kvn[1] = first_weights(3, mine).astype(F32)
    for c in qcopies:
        c.wait()
    scatter_queries(lambda h: qrecv[h // 2, h % 2], qs, heads, rows)
    loads1 = [pltpu.make_async_copy(kc_hbm.at[1], k1, csem.at[0]), pltpu.make_async_copy(vc_hbm.at[1], v1, csem.at[1])]
    base = m * rows
    gives = []
    for g in range(2):
        for c in loads0[g]:
            c.wait()
        attend_rows(range(g * half, (g + 1) * half), heads, lambda b: len_ref[base + b], k0, v0, qs, (kvn.at[0], kvn.at[1]))
        gather_contexts(ctx, qs, g * half, half, heads)
        c = send(ctx.at[pl.ds((1 - chip) * 4, 4), pl.ds(g * half, half), :],
                 lhs.at[:, pl.ds(g * rows + half, half), :], gsem.at[0, g], gsem.at[1, g], across)
        c.start()
        gives.append(c)
        if g == 0:
            start([load_q1] + load_own)
            load_wo.wait()
            push_wo = send(wos.at[core], wos.at[core], psem.at[0, 0], psem.at[1, 0], mate)
            push_wo.start()
            pass_round(0)
    load_q1.wait()
    push_q1 = send(wq1.at[core], wq1.at[core], psem.at[0, 1], psem.at[1, 1], mate)
    push_q1.start()
    for i in range(2):
        load_own[i].wait()
        to_mate(wof.at[2 * m + i])
    start(loads1)
    to_mate(piece(across_m, rep, 0))
    for s in range(1, subs):
        pass_round(s)
        to_mate(piece(across_m, rep, s))
    for g in range(2):
        for i in range(4):
            lhs[i, g * rows:g * rows + half, :] = ctx[chip * 4 + i, g * half:(g + 1) * half, :]
    push_wo.wait()
    ycopies = []
    for g in range(2):
        gives[g].wait()
        both = slice(g * rows, (g + 1) * rows)
        for j in range(chunks):
            y = dot(lhs[0, both, :], wos[0, 0:256, j * 256:(j + 1) * 256])
            for i in range(1, 4):
                y += dot(lhs[i, both, :], wos[i // 2, (i % 2) * 256:(i % 2 + 1) * 256, j * 256:(j + 1) * 256])
            ys[j, both, :] = y
            if j % YSTEP == YSTEP - 1:
                n = len(ycopies)
                part = pl.ds(j + 1 - YSTEP, YSTEP)
                c = send(ys.at[part, pl.ds(g * rows + half, half)], yrecv.at[part, pl.ds(g * half, half)],
                         ysem.at[0, n], ysem.at[1, n], across)
                c.start()
                ycopies.append(c)
    loads_kv = [[pltpu.make_async_copy(src.at[1, pl.ds(j * dim, dim)], wos.at[0, pl.ds(n * dim, dim), pl.ds(j * dim, dim)],
                                       lsem.at[4 + n, j]) for j in range(chunks)] for n, src in enumerate((wk_hbm, wv_hbm))]
    for c in loads_kv[0] + loads_kv[1]:
        c.start()
    for c in around:
        c.wait_recv()
    for s in range(subs):
        n, peer, other = ((1, next_z, rep_y), (0, next_y, rep_z))[s % 2]
        ref = piece(across_m, other, s)
        c = send(ref, ref, yzsem.at[0, n, subs + s // 2], yzsem.at[1, n, subs + s // 2], peer)
        c.start()
        around.append(c)
    for other in (rep_y, rep_z):
        for s in range(subs):
            to_mate(piece(across_m, other, s))
    hcopies = []
    for g in range(2):
        for j in range(chunks):
            if j % YSTEP == 0:
                ycopies[(g * chunks + j) // YSTEP].wait_recv()
            part = slice(g * half, (g + 1) * half)
            old = xs[pl.ds(pl.multiple_of(m * rows + g * half, half), half), j * 256:(j + 1) * 256]
            hl[j, part, :] = (old.astype(F32) + (ys[j, g * rows:g * rows + half, :] + yrecv[j, part, :])).astype(BF16)
            if j % HSTEP == HSTEP - 1:
                n = len(hcopies)
                these = pl.ds(j + 1 - HSTEP, HSTEP)
                c = send(hl.at[these, pl.ds(g * half, half)], hl.at[these, pl.ds(rows + g * half, half)],
                         hsem.at[0, n], hsem.at[1, n], across)
                c.start()
                hcopies.append(c)
    push_q1.wait()
    for j in range(chunks):
        if j % HSTEP == 0:
            for g in range(2):
                hcopies[(g * chunks + j) // HSTEP].wait_recv()
        for i in range(4):
            part = dot(hl[j], wq1[i // 2, j * 256:(j + 1) * 256, (i % 2) * 256:(i % 2 + 1) * 256])
            if j == 0:
                qacc[i] = part
            else:
                qacc[i] += part
    q1copies = []
    for i in range(4):
        q1own[i] = qacc[i].astype(BF16)
        c = send(q1own.at[i, pl.ds(rows, rows)], q1recv.at[i], q1sem.at[0, i], q1sem.at[1, i], across)
        c.start()
        q1copies.append(c)
    for n in range(2):
        for j in range(chunks):
            loads_kv[n][j].wait()
            part = dot(hl[j, 0:rows, :], wos[0, n * dim:(n + 1) * dim, j * dim:(j + 1) * dim])
            t = part if j == 0 else t + part
        kvn[2 + n] = t.astype(BF16).astype(F32)
    for i in range(4):
        q_out[chip * 4 + i] = q1own[i, 0:rows, :]
    for s in range(subs):
        around[2 * subs + s].wait_recv()
    for s in range(subs):
        to_mate(piece(across_m, rep_yz, s))
    for i in range(4):
        q1copies[i].wait_recv()
        q_out[(1 - chip) * 4 + i] = q1recv[i]
    for c in mcopies:
        c.wait()
    for c in xcopies + around + ycopies + hcopies + q1copies:
        c.wait_send()
    for c in loads1:
        c.wait()


PARTS = 4


def write_out(buf, out, layer, sems):
    copies = []
    count = buf.shape[0] // PARTS
    for i in range(PARTS):
        part = pl.ds(i * count, count)
        c = pltpu.make_async_copy(buf.at[part], out.at[layer, part], sems.at[i])
        c.start()
        copies.append(c)
    return copies


def write1_kernel(k1, v1, _k, _v, ko, vo, osem):
    for c in write_out(k1, ko, 1, osem.at[0]) + write_out(v1, vo, 1, osem.at[1]):
        c.wait()


def attend1_kernel(len_ref, q_ref, kvn, k0, v0, k1, v1, ctx, _k0, _v0, _k1, _v1, ko, vo, qs, osem):
    heads, rows, dim = q_ref.shape
    base = lax.axis_index("model") * rows
    tile = 16
    outs = []
    for n, buf in enumerate((k0, v0, k1, v1)):
        def patch(b, carry):
            ln = len_ref[base + b]
            start = pl.multiple_of((ln // tile) * tile, tile)
            hit = lax.broadcasted_iota(jnp.int32, (tile, dim), 0) == ln - start
            old = buf[b, pl.ds(start, tile), :].astype(F32)
            buf[b, pl.ds(start, tile), :] = jnp.where(hit, kvn[n, pl.ds(b, 1), :], old).astype(BF16)
            return carry

        lax.fori_loop(0, rows, patch, 0, unroll=8)
        if n < 2:
            outs += write_out(buf, (ko, vo)[n], 0, osem.at[n])
    scatter_queries(lambda h: q_ref[h], qs, heads, rows)
    attend_rows(range(rows), heads, lambda b: len_ref[base + b], k1, v1, qs)
    gather_contexts(ctx, qs, 0, rows, heads)
    for c in outs:
        c.wait()


def last_kernel(ctx, other, hid, wof, out, left, hl, pl2, hsem, psem):
    rep, m, core, chip = place()
    across_m, mate_m, diag_m = 3 - m, m + 1 - 2 * core, lax.rem(m + 2, 4)
    across, mate = (rep, across_m), (rep, mate_m)
    heads, rows, dim = ctx.shape
    chunks = hl.shape[0]
    cols = chunks // 2
    greet((across, mate))
    hcopies = []
    pcopies = []

    def to_mate(at):
        n = len(pcopies)
        c = send(hl.at[at], pl2.at[at], psem.at[0, n], psem.at[1, n], mate)
        c.start()
        pcopies.append(c)

    for h in range(heads):
        left[h, 0:rows, :] = ctx[h]
        left[h, rows:2 * rows, :] = other[h]
    for j in range(cols):
        y = dot(left[0], wof[0, :, j * dim:(j + 1) * dim])
        for h in range(1, heads):
            y += dot(left[h], wof[h, :, j * dim:(j + 1) * dim])
        at = chip * cols + j
        hl[at] = (hid[at].astype(F32) + y).astype(BF16)
        if j == 0:
            meet((across, mate))
        for n in range(2):
            c = send(hl.at[at, pl.ds(n * rows, rows)], hl.at[at, pl.ds((1 - n) * rows, rows)],
                     hsem.at[0, n, j], hsem.at[1, n, j], across)
            c.start()
            hcopies.append(c)
        to_mate(at)
    for j in range(cols):
        for n in range(2):
            hcopies[2 * j + n].wait_recv()
        to_mate((1 - chip) * cols + j)

    def put(who, at, value):
        out[pl.ds(pl.multiple_of(who * rows, rows), rows), at * dim:(at + 1) * dim] = value

    for j in range(chunks):
        put(m, j, hl[j, 0:rows, :])
        put(across_m, j, hl[j, rows:2 * rows, :])
    for c in pcopies:
        c.wait_recv()
    for j in range(chunks):
        put(mate_m, j, pl2[j, 0:rows, :])
        put(diag_m, j, pl2[j, rows:2 * rows, :])
    for c in hcopies + pcopies:
        c.wait_send()


def solution(mesh):
    row_axes = ("replica", "model")
    cache_spec = P(None, row_axes, None, None)

    def device_step(x, cache_len, w_query, w_key, w_value, w_out, k_cache, v_cache):
        layers, rows, seq, dim = k_cache.shape
        total, width = x.shape
        chunks = width // dim
        local = w_query.shape[-1]
        heads = local // dim * mesh.shape["model"]
        hd = (heads, rows, dim)
        x, cache_len, w_query, w_key, w_value, w_out, k_cache, v_cache = (
            pltpu.with_memory_space_constraint(a, pltpu.HBM)
            for a in (x, cache_len, w_query, w_key, w_value, w_out, k_cache, v_cache))
        remote = functools.partial(pltpu.CompilerParams, has_side_effects=True)
        cache = pltpu.VMEM((rows, seq, dim), BF16)
        qs = pltpu.VMEM((2, rows * heads, 128), F32)

        q, kvn, hid, wof, *caches = pl.pallas_call(
            layer0_kernel,
            out_shape=(pltpu.VMEM(hd, BF16), pltpu.VMEM((4, rows, dim), F32), pltpu.VMEM((chunks, 2 * rows, dim), BF16),
                       pltpu.VMEM((heads, dim, width // 2), BF16)) + (cache,) * 4,
            in_specs=[SM] + [HBM] * 7,
            out_specs=(VM,) * 8,
            scratch_shapes=[
                pltpu.VMEM((total, width), BF16),
                pltpu.VMEM((4, 2, rows, dim), BF16), pltpu.VMEM((4, 2, rows, dim), BF16),
                qs, pltpu.VMEM(hd, BF16),
                pltpu.VMEM((2, local, width), BF16), pltpu.VMEM((4, 2 * rows, dim), BF16),
                pltpu.VMEM((chunks, 2 * rows, dim), F32), pltpu.VMEM((chunks, rows, dim), F32),
                pltpu.VMEM((2, width, local), BF16),
                pltpu.VMEM((4, 2 * rows, dim), F32), pltpu.VMEM((4, 2 * rows, dim), BF16),
                pltpu.VMEM((4, rows, dim), BF16), pltpu.VMEM((local // 4, width // 2), BF16),
                DMA((10,)), DMA((6, 8)), DMA((2, 2)), DMA((2,)), DMA((2, 3, 2)), DMA((2, 2)), DMA((2, 2)), DMA((2, 2 * chunks)), DMA((2, 2 * chunks)),
                DMA((2, 4)), DMA((2, 4)), DMA((2, 2, 6)), DMA((2, 18)),
            ],
            compiler_params=remote(collective_id=0, vmem_limit_bytes=11 << 20),
            name="layer0",
        )(cache_len, x, w_query, w_key, w_value, w_out, k_cache, v_cache)

        ctx, _, _, k1, v1, ko, vo = pl.pallas_call(
            attend1_kernel,
            out_shape=(pltpu.VMEM(hd, BF16), cache, cache, cache, cache,
                       jax.ShapeDtypeStruct(k_cache.shape, BF16), jax.ShapeDtypeStruct(v_cache.shape, BF16)),
            in_specs=[SM] + [VM] * 6,
            out_specs=(VM,) * 5 + (HBM, HBM),
            input_output_aliases={3: 1, 4: 2, 5: 3, 6: 4},
            scratch_shapes=[qs, DMA((2, PARTS))],
            compiler_params=pltpu.CompilerParams(vmem_limit_bytes=3 << 20),
            name="attend1",
        )(cache_len, q, kvn, *caches)

        other = lax.ppermute(ctx, "model", [(i, 3 - i) for i in range(4)])
        ko, vo = pl.pallas_call(
            write1_kernel,
            out_shape=(jax.ShapeDtypeStruct(k_cache.shape, BF16), jax.ShapeDtypeStruct(v_cache.shape, BF16)),
            in_specs=[VM, VM, HBM, HBM],
            out_specs=(HBM, HBM),
            input_output_aliases={2: 0, 3: 1},
            scratch_shapes=[DMA((2, PARTS))],
            compiler_params=pltpu.CompilerParams(vmem_limit_bytes=1 << 20),
            cost_estimate=pl.CostEstimate(flops=10 ** 9, bytes_accessed=2 ** 25, transcendentals=0),
            name="write1",
        )(k1, v1, ko, vo)

        out = pl.pallas_call(
            last_kernel,
            out_shape=pltpu.VMEM((total, width), BF16),
            in_specs=[VM] * 4,
            out_specs=VM,
            scratch_shapes=[
                pltpu.VMEM((heads, 2 * rows, dim), BF16),
                pltpu.VMEM((chunks, 2 * rows, dim), BF16), pltpu.VMEM((chunks, 2 * rows, dim), BF16),
                DMA((2, 2, chunks // 2)), DMA((2, chunks)),
            ],
            compiler_params=remote(collective_id=1, vmem_limit_bytes=4 << 20),
            name="last",
        )(ctx, other, hid, wof)
        return out, ko, vo

    return jax.shard_map(
        device_step,
        mesh=mesh,
        in_specs=(P("replica", None), P("replica"), P(None, None, "model"), P(), P(), P(None, "model", None), cache_spec, cache_spec),
        out_specs=(P("replica", None), cache_spec, cache_spec),
        check_vma=False,
    )
```
